8 devices in a mesh: dp: 2 (over z, y), cp: 4 (over x, core).
Axes of the slice: x: 2, y: 2, z: 1, core: 2. Of those that a mesh axis runs over, the one named last changes fastest.
Arguments:
- q_tok: bfloat16 [4096, 6, 128], P(('dp', 'cp')), parts along dimension 0
- k_tok: bfloat16 [4096, 128], P(('dp', 'cp')), parts along dimension 0
- v_tok: bfloat16 [4096, 128], P(('dp', 'cp')), parts along dimension 0
- fwd_out: bfloat16 [4096, 6, 128], P(('dp', 'cp')), parts along dimension 0
- d_out: bfloat16 [4096, 6, 128], P(('dp', 'cp')), parts along dimension 0
- lse_row: float32 [4096, 6], P(('dp', 'cp')), parts along dimension 0
Outputs:
- output 1: bfloat16 [4096, 6, 128], P(('dp', 'cp')), parts along dimension 0
- output 2: bfloat16 [4096, 128], P(('dp', 'cp')), parts along dimension 0
- output 3: bfloat16 [4096, 128], P(('dp', 'cp')), parts along dimension 0
There are 2 independent parts. The reference program is written for one: setup_inputs(seed, part) draws one part's arguments, and reference() takes and returns one part's arrays. A program takes and returns all parts, laid end to end along the dimension named above; each array names one.
All inputs are finite; a program needn't handle non-finite values.
Results may differ from the reference program's by a relative error of at most 0.001.
Values are sent between devices in bfloat16 or wider.
A program may use at most 1 GiB of HBM per device.

```python
import jax
import jax.numpy as jnp
from jax import lax

TOK_DEV = 512
CP = 4
GQA = 6
HEAD = 128

SEQ = CP * TOK_DEV
Q_BLOCK = min(TOK_DEV, 128)
SOFTMAX_SCALE = HEAD ** -0.5
GRAD_GAIN = 0.25 * SEQ ** 0.5


def attention_forward(q_tok, k_tok, v_tok):
    k_full = k_tok.astype(jnp.float32)
    v_full = v_tok.astype(jnp.float32)
    columns = jnp.arange(SEQ)
    n_blocks = SEQ // Q_BLOCK

    def one_block(block_in):
        q_block, row_ids = block_in
        logits = jnp.einsum('rgd,cd->rgc', q_block.astype(jnp.float32), k_full) * SOFTMAX_SCALE
        allowed = columns[None, :] <= row_ids[:, None]
        logits = jnp.where(allowed[:, None, :], logits, -jnp.inf)
        lse_block = jax.nn.logsumexp(logits, axis=-1)
        prob_mat = jnp.exp(logits - lse_block[:, :, None])
        out_block = jnp.einsum('rgc,cd->rgd', prob_mat, v_full)
        return out_block.astype(jnp.bfloat16), lse_block

    out_blocks, lse_blocks = lax.map(one_block, (q_tok.reshape(n_blocks, Q_BLOCK, GQA, HEAD), columns.reshape(n_blocks, Q_BLOCK)))
    return out_blocks.reshape(SEQ, GQA, HEAD), lse_blocks.reshape(SEQ, GQA)


def setup_inputs(seed: int = 0, part: int = 0) -> dict:
    base_key = jax.random.fold_in(jax.random.key(seed), part)
    key_q, key_k, key_v, key_m, key_g = jax.random.split(base_key, 5)
    q_tok = jax.random.normal(key_q, (SEQ, GQA, HEAD), jnp.float32).astype(jnp.bfloat16)
    k_tok = jax.random.normal(key_k, (SEQ, HEAD), jnp.float32).astype(jnp.bfloat16)
    v_mean = jax.random.normal(key_m, (HEAD,), jnp.float32)
    v_tok = (v_mean[None, :] + jax.random.normal(key_v, (SEQ, HEAD), jnp.float32)).astype(jnp.bfloat16)
    d_out = (GRAD_GAIN * jax.random.normal(key_g, (SEQ, GQA, HEAD), jnp.float32)).astype(jnp.bfloat16)
    fwd_out, lse_row = attention_forward(q_tok, k_tok, v_tok)
    return {'q_tok': q_tok, 'k_tok': k_tok, 'v_tok': v_tok, 'fwd_out': fwd_out, 'd_out': d_out, 'lse_row': lse_row}


def reference(q_tok, k_tok, v_tok, fwd_out, d_out, lse_row):
    row_delta = jnp.sum(d_out.astype(jnp.float32) * fwd_out.astype(jnp.float32), axis=-1)
    k_full = k_tok.astype(jnp.float32)
    v_full = v_tok.astype(jnp.float32)
    columns = jnp.arange(SEQ)
    n_blocks = SEQ // Q_BLOCK

    def one_block(carry, block_in):
        dk_acc, dv_acc = carry
        q_block, do_block, lse_block, delta_block, row_ids = block_in
        q_wide = q_block.astype(jnp.float32)
        do_wide = do_block.astype(jnp.float32)
        logits = jnp.einsum('rgd,cd->rgc', q_wide, k_full) * SOFTMAX_SCALE
        allowed = columns[None, :] <= row_ids[:, None]
        prob_mat = jnp.exp(jnp.where(allowed[:, None, :], logits - lse_block[:, :, None], -jnp.inf))
        d_prob = jnp.einsum('rgd,cd->rgc', do_wide, v_full)
        d_score = prob_mat * (d_prob - delta_block[:, :, None])
        prob_low = prob_mat.astype(jnp.bfloat16).astype(jnp.float32)
        score_low = d_score.astype(jnp.bfloat16).astype(jnp.float32)
        dq_block = jnp.einsum('rgc,cd->rgd', score_low, k_full) * SOFTMAX_SCALE
        dk_acc = dk_acc + jnp.einsum('rgc,rgd->cd', score_low, q_wide)
        dv_acc = dv_acc + jnp.einsum('rgc,rgd->cd', prob_low, do_wide)
        return (dk_acc, dv_acc), dq_block.astype(jnp.bfloat16)

    acc_start = (jnp.zeros((SEQ, HEAD), jnp.float32), jnp.zeros((SEQ, HEAD), jnp.float32))
    block_inputs = (q_tok.reshape(n_blocks, Q_BLOCK, GQA, HEAD), d_out.reshape(n_blocks, Q_BLOCK, GQA, HEAD), lse_row.reshape(n_blocks, Q_BLOCK, GQA), row_delta.reshape(n_blocks, Q_BLOCK, GQA), columns.reshape(n_blocks, Q_BLOCK))
    (dk_acc, dv_acc), dq_blocks = lax.scan(one_block, acc_start, block_inputs)
    grad_q = dq_blocks.reshape(SEQ, GQA, HEAD)
    grad_k = (dk_acc * SOFTMAX_SCALE).astype(jnp.bfloat16)
    grad_v = dv_acc.astype(jnp.bfloat16)
    return (grad_q, grad_k, grad_v)
```

```python
import functools

import jax
import jax.numpy as jnp
from jax import lax
from jax.experimental import pallas as pl
from jax.experimental.pallas import tpu as pltpu
from jax.sharding import PartitionSpec as P

F32 = jnp.float32
BF16 = jnp.bfloat16
MESH = pl.DeviceIdType.MESH
T = 512
G = 6
E = 128
W = 256
SCALE = E ** -0.5
LOG2E = 1.4426950408889634


def dot(a, b, ca, cb):
    return lax.dot_general(a, b, (((ca,), (cb,)), ((), ())), preferred_element_type=F32)


def kernel(q_hbm, k_hbm, v_hbm, o_hbm, do_hbm, lse_hbm, gq_ref, gk_ref, gv_ref,
           q_v, do_v, o_v, lse_v, lcol, dcol, kv, acc, dq, dqr, lr, cr, fr, ld, ss, rs):
    dp = lax.axis_index('dp')
    me = lax.axis_index('cp')
    chip = me // 2
    odd = me - 2 * chip
    even_dev = 2 * chip
    odd_dev = 2 * chip + 1

    def rcopy(i, src, dst, dev):
        return pltpu.make_async_remote_copy(src, dst, ss.at[i], rs.at[i], device_id=(dp, dev), device_id_type=MESH)

    loads = []
    for c in range(2):
        for n, ref in enumerate((k_hbm, v_hbm)):
            loads.append(pltpu.make_async_copy(ref.at[pl.ds(c * W, W)], kv.at[2 * me + c, n], ld.at[2 * c + n]))
    loads.append(pltpu.make_async_copy(lse_hbm, lse_v.at[0], ld.at[4]))
    for n, (ref, buf) in enumerate(((do_hbm, do_v), (o_hbm, o_v), (q_hbm, q_v))):
        loads.append(pltpu.make_async_copy(ref, buf.at[pl.ds(0, G * T)], ld.at[5 + n]))
    for cp in loads:
        cp.start()

    bar = pltpu.get_barrier_semaphore()
    for d in range(1, 4):
        pl.semaphore_signal(bar, 1, device_id=(dp, lax.rem(me + d, 4)), device_id_type=MESH)
    pl.semaphore_wait(bar, 3)

    own = pl.ds(2 * me, 2)
    even_kv = pl.ds(2 * even_dev, 2)
    HALF = pl.ds(G * T // 2, G * T // 2)
    MOVED = pl.ds(G * T, G * T // 2)

    kv_pair = rcopy(0, kv.at[even_kv], kv.at[even_kv], odd_dev)
    q_moved = rcopy(1, q_hbm.at[HALF], q_v.at[MOVED], even_dev)
    do_moved = rcopy(2, do_hbm.at[HALF], do_v.at[MOVED], even_dev)
    o_moved = rcopy(3, o_hbm.at[HALF], o_v.at[MOVED], even_dev)
    lse_moved = rcopy(4, lse_hbm, lse_v.at[1], even_dev)
    kv_x = [rcopy(5 + j, kv.at[pl.ds(2 * j, 2)], kv.at[pl.ds(2 * j, 2)], 3) for j in range(2)]
    kv_f = [rcopy(7 + j, kv.at[pl.ds(2 * j, 2)], kv.at[pl.ds(2 * j, 2)], 2) for j in range(2)]
    dq_back = rcopy(9, dq.at[MOVED], dqr, odd_dev)
    local_back = rcopy(10, acc.at[even_kv], lr, even_dev)
    chip_sum = [rcopy(11 + j, acc.at[pl.ds(2 * j, 2)], cr.at[j], 3) for j in range(2)]
    cross_back = [rcopy(13 + j, acc.at[pl.ds(2 * j, 2)], fr, j) for j in range(2)]

    @pl.when(odd == 1)
    def _():
        do_moved.start()
        o_moved.start()
        lse_moved.start()
        q_moved.start()

    for cp in loads[:4]:
        cp.wait()

    @pl.when(odd == 0)
    def _():
        kv_pair.start()

    @pl.when(me == 0)
    def _():
        kv_x[0].start()

    acc[...] = jnp.zeros_like(acc)
    dq[...] = jnp.zeros_like(dq)
    for cp in loads[4:]:
        cp.wait()

    @pl.when(odd == 0)
    def _():
        do_moved.wait_recv()
        o_moved.wait_recv()
        lse_moved.wait_recv()
        q_moved.wait_recv()

    @pl.when(odd == 1)
    def _():
        lse_v[1, 3:6, :] = lse_v[0, 0:3, :]
        kv_pair.wait_recv()

    def rows_setup(slot, head, rows):
        lse_col = jnp.transpose(lse_v[slot, :, :])[:, head:head + 1] * LOG2E
        delta = jnp.sum(do_v[rows, :].astype(F32) * o_v[rows, :].astype(F32), axis=1, keepdims=True)
        lcol[rows, :] = lse_col
        dcol[rows, :] = delta
        return lse_col, delta

    def scores(q, do, k, v, lse_col, delta, mask=None):
        p = jnp.exp2(dot(q, k, 1, 1) * (SCALE * LOG2E) - lse_col)
        if mask is not None:
            p = jnp.where(mask, p, 0.0)
        ds = p * (dot(do, v, 1, 1) - delta)
        return p.astype(BF16), ds.astype(BF16)

    def full_step(row0, heads, g0, setup_slot=None, head0=0):
        k = jnp.concatenate([kv[g0, 0], kv[g0 + 1, 0]], axis=0)
        v = jnp.concatenate([kv[g0, 1], kv[g0 + 1, 1]], axis=0)
        for h in range(heads):
            rows = pl.ds(pl.multiple_of(row0 + h * T, T), T)
            if setup_slot is None:
                lse_col, delta = lcol[rows, :], dcol[rows, :]
            else:
                lse_col, delta = rows_setup(setup_slot, head0 + h, rows)
            q, do = q_v[rows, :], do_v[rows, :]
            p, ds = scores(q, do, k, v, lse_col, delta)
            dv = dot(do, p, 0, 0)
            dk = dot(q, ds, 0, 0)
            for c in range(2):
                acc[g0 + c, 0] += dk[:, c * W:(c + 1) * W]
                acc[g0 + c, 1] += dv[:, c * W:(c + 1) * W]
            dq[rows, :] += dot(ds, k, 1, 0)

    def diag_step():
        g0 = 2 * me
        k0, k1, v0, v1 = kv[g0, 0], kv[g0 + 1, 0], kv[g0, 1], kv[g0 + 1, 1]
        row_i = lax.broadcasted_iota(jnp.int32, (T, W), 0)
        col_i = lax.broadcasted_iota(jnp.int32, (T, W), 1)
        mask = col_i <= row_i
        for h in range(G):
            rows = pl.ds(h * T, T)
            low = pl.ds(h * T + W, W)
            lse_col, delta = rows_setup(0, h, rows)
            q, do = q_v[rows, :], do_v[rows, :]
            p0, ds0 = scores(q, do, k0, v0, lse_col, delta, mask)
            p1, ds1 = scores(q[W:], do[W:], k1, v1, lse_col[W:], delta[W:], mask[:W])
            acc[g0, 0] += dot(q, ds0, 0, 0)
            acc[g0, 1] += dot(do, p0, 0, 0)
            acc[g0 + 1, 0] += dot(q[W:], ds1, 0, 0)
            acc[g0 + 1, 1] += dot(do[W:], p1, 0, 0)
            dq[rows, :] += dot(ds0, k0, 1, 0)
            dq[low, :] += dot(ds1, k1, 1, 0)

    full_step((1 - odd) * (G * T), G // 2, 2 * even_dev, setup_slot=1, head0=3)

    @pl.when(odd == 0)
    def _():
        dq_back.start()

    @pl.when(odd == 1)
    def _():
        local_back.start()

    @pl.when(me == 1)
    def _():
        kv_x[1].start()

    diag_step()

    @pl.when(chip == 1)
    def _():
        for j in range(2):
            @pl.when(odd == 1)
            def _():
                kv_x[j].wait_recv()
                kv_f[j].start()

            @pl.when(odd == 0)
            def _():
                kv_f[j].wait_recv()

            full_step(0, G, 2 * j)

            @pl.when(odd == 0)
            def _():
                chip_sum[j].start()

            @pl.when(odd == 1)
            def _():
                chip_sum[j].wait_recv()
                acc[2 * j:2 * j + 2] += cr[j]
                cross_back[j].start()

    @pl.when(odd == 1)
    def _():
        dq_back.wait_recv()
        dq[HALF, :] += dqr[...]

    gq_ref[...] = (dq[0:G * T, :] * SCALE).astype(BF16)

    @pl.when(odd == 0)
    def _():
        local_back.wait_recv()
        acc[own] += lr[...]

    @pl.when(me == 0)
    def _():
        cross_back[0].wait_recv()

    @pl.when(me == 1)
    def _():
        cross_back[1].wait_recv()

    @pl.when(chip == 0)
    def _():
        acc[own] += fr[...]

    for c in range(2):
        gk_ref[c * W:(c + 1) * W, :] = jnp.transpose(acc[2 * me + c, 0] * SCALE).astype(BF16)
        gv_ref[c * W:(c + 1) * W, :] = jnp.transpose(acc[2 * me + c, 1]).astype(BF16)

    @pl.when(odd == 0)
    def _():
        kv_pair.wait_send()
        dq_back.wait_send()

    @pl.when(odd == 1)
    def _():
        for cp in (q_moved, do_moved, o_moved, lse_moved, local_back):
            cp.wait_send()

    @pl.when(me == 0)
    def _():
        kv_x[0].wait_send()

    @pl.when(me == 1)
    def _():
        kv_x[1].wait_send()

    @pl.when(me == 2)
    def _():
        for j in range(2):
            chip_sum[j].wait_send()

    @pl.when(me == 3)
    def _():
        for j in range(2):
            kv_f[j].wait_send()
            cross_back[j].wait_send()


def solution(mesh):
    row_spec = P(('dp', 'cp'))
    vmem = pl.BlockSpec(memory_space=pltpu.VMEM)
    hbm = pl.BlockSpec(memory_space=pl.ANY)
    ext = G * T * 3 // 2

    def local_fn(q_tok, k_tok, v_tok, fwd_out, d_out, lse_row):
        def flat(x):
            return jnp.transpose(x, (1, 0, 2)).reshape(G * T, E)

        gq, gk, gv = pl.pallas_call(
            kernel,
            out_shape=(jax.ShapeDtypeStruct((G * T, E), BF16), jax.ShapeDtypeStruct((T, E), BF16), jax.ShapeDtypeStruct((T, E), BF16)),
            in_specs=[hbm] * 6,
            out_specs=(vmem, vmem, vmem),
            scratch_shapes=[
                pltpu.VMEM((ext, E), BF16), pltpu.VMEM((ext, E), BF16), pltpu.VMEM((ext, E), BF16),
                pltpu.VMEM((2, G, T), F32), pltpu.VMEM((ext, 1), F32), pltpu.VMEM((ext, 1), F32),
                pltpu.VMEM((8, 2, W, E), BF16), pltpu.VMEM((8, 2, E, W), F32), pltpu.VMEM((ext, E), F32),
                pltpu.VMEM((G * T // 2, E), F32), pltpu.VMEM((2, 2, E, W), F32), pltpu.VMEM((2, 2, 2, E, W), F32),
                pltpu.VMEM((2, 2, E, W), F32),
                pltpu.SemaphoreType.DMA((8,)), pltpu.SemaphoreType.DMA((15,)), pltpu.SemaphoreType.DMA((15,)),
            ],
            compiler_params=pltpu.CompilerParams(collective_id=0, has_side_effects=True, vmem_limit_bytes=60 * 2 ** 20),
            name='attention_backward',
        )(flat(q_tok), k_tok, v_tok, flat(fwd_out), flat(d_out), lse_row.T)
        return jnp.transpose(gq.reshape(G, T, E), (1, 0, 2)), gk, gv

    return jax.shard_map(local_fn, mesh=mesh, in_specs=(row_spec,) * 6, out_specs=(row_spec,) * 3, check_vma=False)
```

```python
import functools

import jax
import jax.numpy as jnp
from jax import lax
from jax.experimental import pallas as pl
from jax.experimental.pallas import tpu as pltpu
from jax.sharding import PartitionSpec as P

F32 = jnp.float32
BF16 = jnp.bfloat16
MESH = pl.DeviceIdType.MESH
T = 512
G = 6
E = 128
W = 256
SCALE = E ** -0.5
LOG2E = 1.4426950408889634


def dot(a, b, ca, cb):
    return lax.dot_general(a, b, (((ca,), (cb,)), ((), ())), preferred_element_type=F32)


def kernel(q_hbm, k_hbm, v_hbm, o_hbm, do_hbm, lse_hbm, gq_ref, gk_ref, gv_ref,
           q_v, do_v, o_v, lse_v, lcol, dcol, kv, acc, dq, dqr, lr, cr, pr, fr, fs, fb, ld, ss, rs):
    dp = lax.axis_index('dp')
    me = lax.axis_index('cp')
    chip = me // 2
    odd = me - 2 * chip
    even_dev = 2 * chip
    odd_dev = 2 * chip + 1
    scope = jax.named_scope

    def rcopy(i, src, dst, dev):
        return pltpu.make_async_remote_copy(src, dst, ss.at[i], rs.at[i], device_id=(dp, dev), device_id_type=MESH)

    loads = []
    for c in range(2):
        for n, ref in enumerate((k_hbm, v_hbm)):
            loads.append(pltpu.make_async_copy(ref.at[pl.ds(c * W, W)], kv.at[2 * me + c, n], ld.at[2 * c + n]))
    loads.append(pltpu.make_async_copy(lse_hbm, lse_v.at[0], ld.at[4]))
    for n, (ref, buf) in enumerate(((do_hbm, do_v), (o_hbm, o_v), (q_hbm, q_v))):
        loads.append(pltpu.make_async_copy(ref, buf.at[pl.ds(0, G * T)], ld.at[5 + n]))
    for cp in loads:
        cp.start()

    bar = pltpu.get_barrier_semaphore()
    for d in range(1, 4):
        pl.semaphore_signal(bar, 1, device_id=(dp, lax.rem(me + d, 4)), device_id_type=MESH)
    with scope('barrier'):
        pl.semaphore_wait(bar, 3)

    own = pl.ds(2 * me, 2)
    even_kv = pl.ds(2 * even_dev, 2)
    HALF = pl.ds(G * T // 2, G * T // 2)
    MOVED = pl.ds(G * T, G * T // 2)

    kv_pair = rcopy(0, kv.at[even_kv], kv.at[even_kv], odd_dev)
    moved = [rcopy(1, do_hbm.at[HALF], do_v.at[MOVED], even_dev), rcopy(2, o_hbm.at[HALF], o_v.at[MOVED], even_dev),
             rcopy(3, q_hbm.at[HALF], q_v.at[MOVED], even_dev), rcopy(4, lse_hbm, lse_v.at[1], even_dev)]
    kv_x = [rcopy(5 + g, kv.at[g], kv.at[g], 3) for g in range(4)]
    kv_f = [rcopy(9 + g, kv.at[g], kv.at[g], 2) for g in range(4)]
    dq_back = rcopy(13, dq.at[MOVED], dqr, odd_dev)
    local_back = rcopy(14, acc.at[even_kv], lr, even_dev)
    chip_sum = [rcopy(15 + g, acc.at[g], cr.at[g], 3) for g in range(4)]
    part = rcopy(19, acc.at[pl.ds(2, 2)], pr, 3)
    back = [rcopy(20 + g, acc.at[g], fr.at[g], 0) for g in range(2)] + [rcopy(22 + g, fs.at[g], fb.at[g], 1) for g in range(2)]

    with scope('wait_kv'):
        for cp in loads[:4]:
            cp.wait()

    @pl.when(odd == 0)
    def _():
        kv_pair.start()

    @pl.when(odd == 1)
    def _():
        for cp in moved:
            cp.start()

    @pl.when(me == 0)
    def _():
        kv_x[0].start()
        kv_x[1].start()

    with scope('zero_wait_loads'):
        acc[...] = jnp.zeros_like(acc)
        dq[...] = jnp.zeros_like(dq)
        for cp in loads[4:]:
            cp.wait()

    def rows_setup(lse_t, head, rows):
        lse_col = lse_t[:, head:head + 1]
        delta = jnp.sum(do_v[rows, :].astype(F32) * o_v[rows, :].astype(F32), axis=1, keepdims=True)
        lcol[rows, :] = lse_col
        dcol[rows, :] = delta
        return lse_col, delta

    def scores(q, do, k, v, lse_col, delta, mask=None):
        p = jnp.exp2(dot(q, k, 1, 1) * (SCALE * LOG2E) - lse_col)
        if mask is not None:
            p = jnp.where(mask, p, 0.0)
        ds = p * (dot(do, v, 1, 1) - delta)
        return p.astype(BF16), ds.astype(BF16)

    def chunk_step(g):
        k, v = kv[g, 0], kv[g, 1]
        for h in range(0, G, 2):
            rows = pl.ds(h * T, 2 * T)
            q, do = q_v[rows, :], do_v[rows, :]
            p, ds = scores(q, do, k, v, lcol[rows, :], dcol[rows, :])
            acc[g, 0] += dot(q, ds, 0, 0)
            acc[g, 1] += dot(do, p, 0, 0)
            dq[rows, :] += dot(ds, k, 1, 0)

    def pair_step(heads):
        row0 = (1 - odd) * (G * T)
        g0 = 2 * even_dev
        lse_t = jnp.transpose(lse_v[1, :, :] * LOG2E)
        k = jnp.concatenate([kv[g0, 0], kv[g0 + 1, 0]], axis=0)
        v = jnp.concatenate([kv[g0, 1], kv[g0 + 1, 1]], axis=0)
        for h in heads:
            rows = pl.ds(pl.multiple_of(row0 + h * T, T), T)
            lse_col, delta = rows_setup(lse_t, 3 + h, rows)
            q, do = q_v[rows, :], do_v[rows, :]
            p, ds = scores(q, do, k, v, lse_col, delta)
            dk = dot(q, ds, 0, 0)
            dv = dot(do, p, 0, 0)
            for c in range(2):
                acc[g0 + c, 0] += dk[:, c * W:(c + 1) * W]
                acc[g0 + c, 1] += dv[:, c * W:(c + 1) * W]
            dq[rows, :] += dot(ds, k, 1, 0)

    def diag_step():
        g0 = 2 * me
        k0, k1, v0, v1 = kv[g0, 0], kv[g0 + 1, 0], kv[g0, 1], kv[g0 + 1, 1]
        row_i = lax.broadcasted_iota(jnp.int32, (T, W), 0)
        col_i = lax.broadcasted_iota(jnp.int32, (T, W), 1)
        mask = col_i <= row_i
        lse_t = jnp.transpose(lse_v[0, :, :] * LOG2E)
        for h in range(G):
            rows = pl.ds(h * T, T)
            low = pl.ds(h * T + W, W)
            lse_col, delta = rows_setup(lse_t, h, rows)
            q, do = q_v[rows, :], do_v[rows, :]
            p0, ds0 = scores(q, do, k0, v0, lse_col, delta, mask)
            p1, ds1 = scores(q[W:], do[W:], k1, v1, lse_col[W:], delta[W:], mask[:W])
            acc[g0, 0] += dot(q, ds0, 0, 0)
            acc[g0, 1] += dot(do, p0, 0, 0)
            acc[g0 + 1, 0] += dot(q[W:], ds1, 0, 0)
            acc[g0 + 1, 1] += dot(do[W:], p1, 0, 0)
            dq[rows, :] += dot(ds0, k0, 1, 0)
            dq[low, :] += dot(ds1, k1, 1, 0)

    def return_chunk(g):
        chip_sum[g].wait_recv()
        if g < 2:
            acc[g] += cr[g]
        else:
            if g == 2:
                part.wait_recv()
            total = acc[g] + cr[g] + pr[g - 2]
            fs[g - 2, 0] = (total[0] * SCALE).astype(BF16)
            fs[g - 2, 1] = total[1].astype(BF16)
        back[g].start()

    with scope('diag'):
        diag_step()

    @pl.when(me == 1)
    def _():
        kv_x[2].start()
        kv_x[3].start()
        part.start()

    @pl.when(chip == 1)
    def _():
        for g in range(4):
            with scope('wait_x'):
                @pl.when(odd == 1)
                def _():
                    kv_x[g].wait_recv()
                    kv_f[g].start()

                @pl.when(odd == 0)
                def _():
                    kv_f[g].wait_recv()

            with scope('cross'):
                chunk_step(g)

            with scope('sum'):
                @pl.when(odd == 0)
                def _():
                    chip_sum[g].start()

                if g > 0:
                    @pl.when(odd == 1)
                    def _():
                        return_chunk(g - 1)

    with scope('wait_pair'):
        @pl.when(odd == 0)
        def _():
            for cp in moved:
                cp.wait_recv()

        @pl.when(odd == 1)
        def _():
            lse_v[1, 3:6, :] = lse_v[0, 0:3, :]
            kv_pair.wait_recv()

    with scope('pair'):
        pair_step((0, 1))

    with scope('return3'):
        @pl.when(me == 3)
        def _():
            return_chunk(3)

    with scope('pair'):
        pair_step((2,))

    @pl.when(odd == 0)
    def _():
        dq_back.start()

    @pl.when(odd == 1)
    def _():
        local_back.start()

    with scope('results'):
        @pl.when(odd == 1)
        def _():
            dq_back.wait_recv()
            dq[HALF, :] += dqr[...]

        gq_ref[...] = (dq[0:G * T, :] * SCALE).astype(BF16)

        @pl.when(odd == 0)
        def _():
            local_back.wait_recv()
            acc[own] += lr[...]

        @pl.when(me == 0)
        def _():
            back[0].wait_recv()
            back[1].wait_recv()
            acc[own] += fr[...]

        @pl.when(me == 1)
        def _():
            for c in range(2):
                back[2 + c].wait_recv()
                gk_ref[c * W:(c + 1) * W, :] = jnp.transpose(fb[c, 0])
                gv_ref[c * W:(c + 1) * W, :] = jnp.transpose(fb[c, 1])

        @pl.when(me != 1)
        def _():
            for c in range(2):
                gk_ref[c * W:(c + 1) * W, :] = jnp.transpose(acc[2 * me + c, 0] * SCALE).astype(BF16)
                gv_ref[c * W:(c + 1) * W, :] = jnp.transpose(acc[2 * me + c, 1]).astype(BF16)

    with scope('sends'):
        @pl.when(odd == 0)
        def _():
            kv_pair.wait_send()
            dq_back.wait_send()

        @pl.when(odd == 1)
        def _():
            for cp in moved + [local_back]:
                cp.wait_send()

        @pl.when(me == 0)
        def _():
            kv_x[0].wait_send()
            kv_x[1].wait_send()

        @pl.when(me == 1)
        def _():
            for cp in (kv_x[2], kv_x[3], part):
                cp.wait_send()

        @pl.when(me == 2)
        def _():
            for g in range(4):
                chip_sum[g].wait_send()

        @pl.when(me == 3)
        def _():
            for g in range(4):
                kv_f[g].wait_send()
                back[g].wait_send()


def write_out(gq_v, gk_v, gv_v, gq_hbm, gk_hbm, gv_hbm, sem):
    copies = [pltpu.make_async_copy(a, b, sem.at[i]) for i, (a, b) in enumerate(((gq_v, gq_hbm), (gk_v, gk_hbm), (gv_v, gv_hbm)))]
    for cp in copies:
        cp.start()
    for cp in copies:
        cp.wait()


def solution(mesh):
    row_spec = P(('dp', 'cp'))
    vmem = pl.BlockSpec(memory_space=pltpu.VMEM)
    hbm = pl.BlockSpec(memory_space=pltpu.HBM)
    ext = G * T * 3 // 2

    def local_fn(q_tok, k_tok, v_tok, fwd_out, d_out, lse_row):
        def flat(x):
            return jnp.transpose(x, (1, 0, 2)).reshape(G * T, E)

        results = (jax.ShapeDtypeStruct((G * T, E), BF16), jax.ShapeDtypeStruct((T, E), BF16), jax.ShapeDtypeStruct((T, E), BF16))
        staged = pl.pallas_call(
            kernel,
            out_shape=results,
            in_specs=[hbm] * 6,
            out_specs=(vmem, vmem, vmem),
            scratch_shapes=[
                pltpu.VMEM((ext, E), BF16), pltpu.VMEM((ext, E), BF16), pltpu.VMEM((ext, E), BF16),
                pltpu.VMEM((2, G, T), F32), pltpu.VMEM((ext, 1), F32), pltpu.VMEM((ext, 1), F32),
                pltpu.VMEM((8, 2, W, E), BF16), pltpu.VMEM((8, 2, E, W), F32), pltpu.VMEM((ext, E), F32),
                pltpu.VMEM((G * T // 2, E), F32), pltpu.VMEM((2, 2, E, W), F32), pltpu.VMEM((4, 2, E, W), F32),
                pltpu.VMEM((2, 2, E, W), F32), pltpu.VMEM((2, 2, E, W), F32), pltpu.VMEM((2, 2, E, W), BF16), pltpu.VMEM((2, 2, E, W), BF16),
                pltpu.SemaphoreType.DMA((8,)), pltpu.SemaphoreType.DMA((24,)), pltpu.SemaphoreType.DMA((24,)),
            ],
            compiler_params=pltpu.CompilerParams(collective_id=0, has_side_effects=True, vmem_limit_bytes=40 * 2 ** 20),
            name='attention_backward',
        )(*[pltpu.with_memory_space_constraint(x, pltpu.HBM) for x in (flat(q_tok), k_tok, v_tok, flat(fwd_out), flat(d_out), lse_row.T)])
        gq, gk, gv = pl.pallas_call(
            write_out,
            out_shape=results,
            in_specs=[vmem] * 3,
            out_specs=(hbm,) * 3,
            scratch_shapes=[pltpu.SemaphoreType.DMA((3,))],
            compiler_params=pltpu.CompilerParams(vmem_limit_bytes=4 * 2 ** 20),
            name='write_out',
        )(*staged)
        return jnp.transpose(gq.reshape(G, T, E), (1, 0, 2)), gk, gv

    return jax.shard_map(local_fn, mesh=mesh, in_specs=(row_spec,) * 6, out_specs=(row_spec,) * 3, check_vma=False)
```

```python
import functools

import jax
import jax.numpy as jnp
from jax import lax
from jax.experimental import pallas as pl
from jax.experimental.pallas import tpu as pltpu
from jax.sharding import PartitionSpec as P

F32 = jnp.float32
BF16 = jnp.bfloat16
MESH = pl.DeviceIdType.MESH
T = 512
G = 6
E = 128
W = 256
SCALE = E ** -0.5
LOG2E = 1.4426950408889634


def dot(a, b, ca, cb):
    return lax.dot_general(a, b, (((ca,), (cb,)), ((), ())), preferred_element_type=F32)


def kernel(q_hbm, k_hbm, v_hbm, o_hbm, do_hbm, lse_hbm, gq_ref, gk_ref, gv_ref,
           x_v, lse_v, lcol, dcol, kv, acc, dq, dqr, lr, cr, pr, fr, fs, fb, ld, ss, rs, go):
    dp = lax.axis_index('dp')
    me = lax.axis_index('cp')
    chip = me // 2
    odd = me - 2 * chip
    even_dev = 2 * chip
    odd_dev = 2 * chip + 1
    scope = jax.named_scope
    do_v, o_v, q_v = x_v.at[0], x_v.at[1], x_v.at[2]

    def rcopy(i, j, src, dst, dev):
        return pltpu.make_async_remote_copy(src, dst, ss.at[i], rs.at[j], device_id=(dp, dev), device_id_type=MESH)

    def when(cond, *fns):
        @pl.when(cond)
        def _():
            for f in fns:
                f()

    mine = pl.ds(me * T, T)
    loads = [pltpu.make_async_copy(src, dst, ld.at[n]) for n, (src, dst) in enumerate((
        (k_hbm, kv.at[0, mine]), (v_hbm, kv.at[1, mine]), (lse_hbm, lse_v.at[0]),
        (do_hbm, do_v.at[pl.ds(0, G * T)]), (o_hbm, o_v.at[pl.ds(0, G * T)]), (q_hbm, q_v.at[pl.ds(0, G * T)])))]
    for cp in loads:
        cp.start()

    bar = pltpu.get_barrier_semaphore()

    def greet(sem, dev):
        pl.semaphore_signal(sem, 1, device_id=(dp, dev), device_id_type=MESH)

    @pl.when(me == 3)
    def _():
        for d in range(3):
            greet(bar, d)

    when(me != 3, lambda: greet(bar, 3))
    with scope('barrier'):
        when(me == 3, lambda: pl.semaphore_wait(bar, 3))
        when(me != 3, lambda: pl.semaphore_wait(bar, 1))

    @pl.when(me == 3)
    def _():
        for d in range(3):
            greet(go, d)

    own = pl.ds(2 * me, 2)
    HALF = pl.ds(G * T // 2, G * T // 2)
    MOVED = pl.ds(G * T, G * T // 2)
    even_rows = pl.ds(even_dev * T, T)

    def kv_chunk(g):
        return kv.at[:, pl.ds(g * W, W)]

    kv_pair = rcopy(0, 0, kv.at[:, even_rows], kv.at[:, even_rows], odd_dev)
    dq_back = rcopy(1, 1, dq.at[MOVED], dqr, odd_dev)
    moved = [rcopy(0, 0, lse_v.at[0], lse_v.at[1], even_dev), rcopy(1, 1, x_v.at[:, HALF], x_v.at[:, MOVED], even_dev)]
    local_back = rcopy(2, 2, acc.at[pl.ds(2 * even_dev, 2)], lr, even_dev)
    kv_x = [rcopy((2, 3, 3, 4)[g], 2 + g, kv_chunk(g), kv_chunk(g), 3) for g in range(4)]
    kv_f = [rcopy(3 + g % 2, 3 + g, kv_chunk(g), kv_chunk(g), 2) for g in range(4)]
    chip_sum = [rcopy(5 + g % 2, 7 + g, acc.at[g], cr.at[g], 2) for g in range(4)]
    part = [rcopy(5 + c, 11 + c, acc.at[2 + c], pr.at[c], 2) for c in range(2)]
    back = [rcopy(2 + g, 3 + g, acc.at[g], fr.at[g], 0) for g in range(2)]
    back += [rcopy(4 + c, 2 + c, fs.at[c], fb.at[c], 1) for c in range(2)]

    with scope('wait_kv'):
        loads[0].wait()
        loads[1].wait()

    when(me == 0, kv_x[0].start, kv_x[1].start)

    with scope('zero_wait_loads'):
        acc[...] = jnp.zeros_like(acc)
        zeros = pl.ds(4 * T, (G - 4) * T + G * T // 2)
        dq[zeros, :] = jnp.zeros((zeros.size, E), F32)
        for cp in loads[2:]:
            cp.wait()

    def rows_setup(lse_t, head, rows):
        lcol[rows, :] = jnp.broadcast_to(lse_t[:, head:head + 1], (T, E))
        delta = jnp.sum(do_v[rows, :].astype(F32) * o_v[rows, :].astype(F32), axis=1, keepdims=True)
        dcol[rows, :] = jnp.broadcast_to(delta, (T, E))

    def scores(q, do, k, v, lse_col, delta, mask=None):
        n = k.shape[0] // E
        p = jnp.exp2(dot(q, k, 1, 1) * (SCALE * LOG2E) - jnp.concatenate([lse_col] * n, axis=1))
        if mask is not None:
            step = p.shape[0] // 2
            p = jnp.concatenate([x for i in range(0, 2 * step, step)
                                 for x in (jnp.where(mask, p[i:i + W], 0.0), p[i + W:i + step])[:step // W]], axis=0)
        ds = p * (dot(do, v, 1, 1) - jnp.concatenate([delta] * n, axis=1))
        return p.astype(BF16), ds.astype(BF16)

    def chunk_step(g):
        cols = pl.ds(g * W, W)
        k, v = kv[0, cols, :], kv[1, cols, :]
        blocks = [pl.ds(h * T, 2 * T) for h in range(0, G, 2)]
        done = [scores(q_v[rows, :], do_v[rows, :], k, v, lcol[rows, :], dcol[rows, :]) for rows in blocks]
        for rows, (p, ds) in zip(blocks, done):
            dq[rows, :] += dot(ds, k, 1, 0)
            acc[g, 0] += dot(q_v[rows, :], ds, 0, 0)
            acc[g, 1] += dot(do_v[rows, :], p, 0, 0)

    def pair_step(heads):
        row0 = (1 - odd) * (G * T)
        g0 = 2 * even_dev
        lse_t = jnp.transpose(lse_v[1, :, :] * LOG2E)
        k, v = kv[0, even_rows, :], kv[1, even_rows, :]
        blocks = [pl.ds(pl.multiple_of(row0 + h * T, T), T) for h in heads]
        for h, rows in zip(heads, blocks):
            rows_setup(lse_t, 3 + h, rows)
        done = [scores(q_v[rows, :], do_v[rows, :], k, v, lcol[rows, :], dcol[rows, :]) for rows in blocks]
        for rows, (p, ds) in zip(blocks, done):
            dq[rows, :] += dot(ds, k, 1, 0)
            dk = dot(q_v[rows, :], ds, 0, 0)
            dv = dot(do_v[rows, :], p, 0, 0)
            for c in range(2):
                acc[g0 + c, 0] += dk[:, c * W:(c + 1) * W]
                acc[g0 + c, 1] += dv[:, c * W:(c + 1) * W]

    def diag_step(heads, setup_heads):
        g0 = 2 * me
        k, v = kv[0, mine, :], kv[1, mine, :]
        row_i = lax.broadcasted_iota(jnp.int32, (W, W), 0)
        col_i = lax.broadcasted_iota(jnp.int32, (W, W), 1)
        mask = col_i <= row_i
        if setup_heads:
            lse_t = jnp.transpose(lse_v[0, :, :] * LOG2E)

        def low(x):
            return jnp.concatenate([x[W:T], x[T + W:]], axis=0)

        for h in heads:
            if setup_heads:
                for i in range(2):
                    rows_setup(lse_t, h + i, pl.ds((h + i) * T, T))
            rows = pl.ds(h * T, 2 * T)
            lse_col, delta = lcol[rows, :], dcol[rows, :]
            q, do = q_v[rows, :], do_v[rows, :]
            p0, ds0 = scores(q, do, k[:W], v[:W], lse_col, delta, mask)
            q1, do1 = low(q), low(do)
            p1, ds1 = scores(q1, do1, k[W:], v[W:], low(lse_col), low(delta), mask)
            dq0, dq1 = dot(ds0, k[:W], 1, 0), dot(ds1, k[W:], 1, 0)
            new = [x for i in range(2) for x in (dq0[i * T:i * T + W], dq0[i * T + W:(i + 1) * T] + dq1[i * W:(i + 1) * W])]
            if h < 4:
                dq[rows, :] = jnp.concatenate(new, axis=0)
            else:
                dq[rows, :] += jnp.concatenate(new, axis=0)
            acc[g0, 0] += dot(q, ds0, 0, 0)
            acc[g0, 1] += dot(do, p0, 0, 0)
            acc[g0 + 1, 0] += dot(q1, ds1, 0, 0)
            acc[g0 + 1, 1] += dot(do1, p1, 0, 0)
        for h in range(max(heads) + 2, setup_heads):
            rows_setup(lse_t, h, pl.ds(h * T, T))

    def return_chunk(g):
        chip_sum[g].wait_recv()
        if g < 2:
            acc[g] += cr[g]
        else:
            part[g - 2].wait_recv()
            total = acc[g] + cr[g] + pr[g - 2]
            fs[g - 2, 0] = (total[0] * SCALE).astype(BF16)
            fs[g - 2, 1] = total[1].astype(BF16)
        back[g].start()

    with scope('diag_a'):
        diag_step((0, 2), G)

    with scope('go'):
        when(me != 3, lambda: pl.semaphore_wait(go, 1))

    when(me == 1, kv_x[2].start, kv_x[3].start)
    when(odd == 0, kv_pair.start)
    when(me == 1, moved[0].start, moved[1].start)

    with scope('diag_b'):
        when(me != 3, lambda: diag_step((4,), 0))

    when(me == 1, part[0].start, part[1].start)

    def forward(g):
        kv_x[g].wait_recv()
        if g >= 2:
            kv_f[g - 2].wait_send()
        kv_f[g].start()

    def send_sum(g):
        if g >= 2:
            chip_sum[g - 2].wait_send()
        chip_sum[g].start()

    @pl.when(chip == 1)
    def _():
        with scope('wait_x'):
            when(odd == 1, lambda: forward(0), moved[0].start, moved[1].start)
        for g in range(4):
            with scope('wait_f'):
                when(odd == 0, kv_f[g].wait_recv)
            with scope('cross'):
                chunk_step(g)
            with scope('sum'):
                @pl.when(odd == 1)
                def _():
                    send_sum(g)
                    if g < 3:
                        forward(g + 1)

                if g < 3:
                    when(odd == 0, lambda: return_chunk(g))

        with scope('diag_b'):
            when(odd == 1, lambda: diag_step((4,), 0))

    with scope('wait_pair'):
        when(odd == 0, moved[0].wait_recv, moved[1].wait_recv)

        @pl.when(odd == 1)
        def _():
            lse_v[1, 3:6, :] = lse_v[0, 0:3, :]
            kv_pair.wait_recv()

    with scope('pair'):
        pair_step((0,))

    with scope('return3'):
        when(me == 2, lambda: return_chunk(3))

    with scope('pair'):
        pair_step((1, 2))

    when(odd == 0, dq_back.start)
    when(odd == 1, local_back.start)

    with scope('results'):
        @pl.when(odd == 1)
        def _():
            dq_back.wait_recv()
            dq[HALF, :] += dqr[...]

        gq_ref[...] = (dq[0:G * T, :] * SCALE).astype(BF16)

        @pl.when(odd == 0)
        def _():
            local_back.wait_recv()
            acc[own] += lr[...]

        @pl.when(me == 0)
        def _():
            back[0].wait_recv()
            back[1].wait_recv()
            acc[own] += fr[...]

        @pl.when(me == 1)
        def _():
            for c in range(2):
                back[2 + c].wait_recv()
                gk_ref[c * W:(c + 1) * W, :] = jnp.transpose(fb[c, 0])
                gv_ref[c * W:(c + 1) * W, :] = jnp.transpose(fb[c, 1])

        @pl.when(me != 1)
        def _():
            for c in range(2):
                gk_ref[c * W:(c + 1) * W, :] = jnp.transpose(acc[2 * me + c, 0] * SCALE).astype(BF16)
                gv_ref[c * W:(c + 1) * W, :] = jnp.transpose(acc[2 * me + c, 1]).astype(BF16)

    with scope('sends'):
        when(odd == 0, kv_pair.wait_send, dq_back.wait_send)
        when(odd == 1, moved[0].wait_send, moved[1].wait_send, local_back.wait_send)
        when(me == 0, kv_x[0].wait_send, kv_x[1].wait_send)
        when(me == 1, kv_x[2].wait_send, kv_x[3].wait_send, part[0].wait_send, part[1].wait_send)
        when(me == 2, *(cp.wait_send for cp in back))
        when(me == 3, kv_f[2].wait_send, kv_f[3].wait_send, chip_sum[2].wait_send, chip_sum[3].wait_send)


def write_out(gq_v, gk_v, gv_v, gq_hbm, gk_hbm, gv_hbm, sem):
    pieces = [pl.ds(i * 2 * T, 2 * T) for i in range(G // 2)]
    pairs = [(gq_v.at[r], gq_hbm.at[r]) for r in pieces] + [(gk_v, gk_hbm), (gv_v, gv_hbm)]
    copies = [pltpu.make_async_copy(a, b, sem.at[i]) for i, (a, b) in enumerate(pairs)]
    for cp in copies:
        cp.start()
    for cp in copies:
        cp.wait()


def solution(mesh):
    row_spec = P(('dp', 'cp'))
    vmem = pl.BlockSpec(memory_space=pltpu.VMEM)
    hbm = pl.BlockSpec(memory_space=pltpu.HBM)
    ext = G * T * 3 // 2

    def local_fn(q_tok, k_tok, v_tok, fwd_out, d_out, lse_row):
        def flat(x):
            return jnp.transpose(x, (1, 0, 2)).reshape(G * T, E)

        results = (jax.ShapeDtypeStruct((G * T, E), BF16), jax.ShapeDtypeStruct((T, E), BF16), jax.ShapeDtypeStruct((T, E), BF16))
        staged = pl.pallas_call(
            kernel,
            out_shape=results,
            in_specs=[hbm] * 6,
            out_specs=(vmem, vmem, vmem),
            scratch_shapes=[
                pltpu.VMEM((3, ext, E), BF16), pltpu.VMEM((2, G, T), F32), pltpu.VMEM((ext, E), F32), pltpu.VMEM((ext, E), F32),
                pltpu.VMEM((2, 4 * T, E), BF16), pltpu.VMEM((8, 2, E, W), F32), pltpu.VMEM((ext, E), F32),
                pltpu.VMEM((G * T // 2, E), F32), pltpu.VMEM((2, 2, E, W), F32), pltpu.VMEM((4, 2, E, W), F32),
                pltpu.VMEM((2, 2, E, W), F32), pltpu.VMEM((2, 2, E, W), F32),
                pltpu.VMEM((2, 2, E, W), BF16), pltpu.VMEM((2, 2, E, W), BF16),
                pltpu.SemaphoreType.DMA((6,)), pltpu.SemaphoreType.DMA((7,)), pltpu.SemaphoreType.DMA((13,)), pltpu.SemaphoreType.REGULAR,
            ],
            compiler_params=pltpu.CompilerParams(collective_id=0, has_side_effects=True, vmem_limit_bytes=40 * 2 ** 20),
            name='attention_backward',
        )(*[pltpu.with_memory_space_constraint(x, pltpu.HBM) for x in (flat(q_tok), k_tok, v_tok, flat(fwd_out), flat(d_out), lse_row.T)])
        gq, gk, gv = pl.pallas_call(
            write_out,
            out_shape=results,
            in_specs=[vmem] * 3,
            out_specs=(hbm,) * 3,
            scratch_shapes=[pltpu.SemaphoreType.DMA((2 + G // 2,))],
            compiler_params=pltpu.CompilerParams(vmem_limit_bytes=4 * 2 ** 20),
            name='write_out',
        )(*staged)
        return jnp.transpose(gq.reshape(G, T, E), (1, 0, 2)), gk, gv

    return jax.shard_map(local_fn, mesh=mesh, in_specs=(row_spec,) * 6, out_specs=(row_spec,) * 3, check_vma=False)
```

```python
import functools

import jax
import jax.numpy as jnp
from jax import lax
from jax.experimental import pallas as pl
from jax.experimental.pallas import tpu as pltpu
from jax.sharding import PartitionSpec as P

F32 = jnp.float32
BF16 = jnp.bfloat16
MESH = pl.DeviceIdType.MESH
T = 512
G = 6
E = 128
W = 256
SCALE = E ** -0.5
LOG2E = 1.4426950408889634


def dot(a, b, ca, cb):
    return lax.dot_general(a, b, (((ca,), (cb,)), ((), ())), preferred_element_type=F32)


def kernel(q_hbm, k_hbm, v_hbm, o_hbm, do_hbm, lse_hbm, gq_ref, gk_ref, gv_ref,
           x_v, lse_v, lcol, dcol, kv, acc, dq, dqr, lr, cr, pr, fr, fs, fb, ld, ss, rs, go):
    dp = lax.axis_index('dp')
    me = lax.axis_index('cp')
    chip = me // 2
    odd = me - 2 * chip
    even_dev = 2 * chip
    odd_dev = 2 * chip + 1
    scope = jax.named_scope
    do_v, o_v, q_v = x_v.at[0], x_v.at[1], x_v.at[2]

    def rcopy(i, j, src, dst, dev):
        return pltpu.make_async_remote_copy(src, dst, ss.at[i], rs.at[j], device_id=(dp, dev), device_id_type=MESH)

    def when(cond, *fns):
        @pl.when(cond)
        def _():
            for f in fns:
                f()

    mine = pl.ds(me * T, T)
    loads = [pltpu.make_async_copy(src, dst, ld.at[n]) for n, (src, dst) in enumerate((
        (k_hbm, kv.at[0, mine]), (v_hbm, kv.at[1, mine]), (lse_hbm, lse_v.at[0]),
        (do_hbm, do_v.at[pl.ds(0, G * T)]), (o_hbm, o_v.at[pl.ds(0, G * T)]), (q_hbm, q_v.at[pl.ds(0, G * T)])))]
    for cp in loads:
        cp.start()

    bar = pltpu.get_barrier_semaphore()

    def greet(sem, dev):
        pl.semaphore_signal(sem, 1, device_id=(dp, dev), device_id_type=MESH)

    @pl.when(me == 3)
    def _():
        for d in range(3):
            greet(bar, d)

    when(me != 3, lambda: greet(bar, 3))
    with scope('barrier'):
        when(me == 3, lambda: pl.semaphore_wait(bar, 3))
        when(me != 3, lambda: pl.semaphore_wait(bar, 1))

    @pl.when(me == 3)
    def _():
        for d in range(3):
            greet(go, d)

    own = pl.ds(2 * me, 2)
    HALF = pl.ds(G * T // 2, G * T // 2)
    MOVED = pl.ds(G * T, G * T // 2)
    even_rows = pl.ds(even_dev * T, T)

    def kv_chunk(g):
        return kv.at[:, pl.ds(g * W, W)]

    kv_pair = rcopy(0, 0, kv.at[:, even_rows], kv.at[:, even_rows], odd_dev)
    dq_back = rcopy(1, 1, dq.at[MOVED], dqr, odd_dev)
    moved = [rcopy(0, 0, lse_v.at[0], lse_v.at[1], even_dev), rcopy(1, 1, x_v.at[:, HALF], x_v.at[:, MOVED], even_dev)]
    local_back = rcopy(2, 2, acc.at[pl.ds(2 * even_dev, 2)], lr, even_dev)
    kv_x = [rcopy((2, 3, 3, 4)[g], 2 + g, kv_chunk(g), kv_chunk(g), 3) for g in range(4)]
    kv_f = [rcopy(3 + g % 2, 3 + g, kv_chunk(g), kv_chunk(g), 2) for g in range(4)]
    first_sum = [rcopy(5 + 2 * n, 7 + 2 * n, acc.at[0, n], cr.at[0, n], 2) for n in range(2)]
    chip_sum = [None, rcopy(6, 8, acc.at[1], cr.at[1], 2)]
    chip_sum += [rcopy(2 + g, 4 + g, acc.at[g], cr.at[g], 3) for g in range(2, 4)]
    part = [rcopy(5 + c, 8 + c, acc.at[2 + c], pr.at[c], 3) for c in range(2)]
    first_back = [rcopy(2 + 4 * n, 3 + 2 * n, acc.at[0, n], fr.at[0, n], 0) for n in range(2)]
    back = [None, rcopy(3, 4, acc.at[1], fr.at[1], 0)]
    back += [rcopy(5 + c, 2 + c, fs.at[c], fb.at[c], 1) for c in range(2)]

    with scope('wait_kv'):
        loads[0].wait()
        loads[1].wait()

    when(me == 0, kv_x[0].start, kv_x[1].start)

    with scope('zero_wait_loads'):
        acc[...] = jnp.zeros_like(acc)
        zeros = pl.ds(4 * T, (G - 4) * T + G * T // 2)
        dq[zeros, :] = jnp.zeros((zeros.size, E), F32)
        for cp in loads[2:]:
            cp.wait()

    def rows_setup(lse_t, head, rows):
        lcol[rows, :] = jnp.broadcast_to(lse_t[:, head:head + 1], (T, E))
        delta = jnp.sum(do_v[rows, :].astype(F32) * o_v[rows, :].astype(F32), axis=1, keepdims=True)
        dcol[rows, :] = jnp.broadcast_to(delta, (T, E))

    def scores(q, do, k, v, lse_col, delta, mask=None):
        n = k.shape[0] // E
        p = jnp.exp2(dot(q, k, 1, 1) * (SCALE * LOG2E) - jnp.concatenate([lse_col] * n, axis=1))
        if mask is not None:
            step = p.shape[0] // 2
            p = jnp.concatenate([x for i in range(0, 2 * step, step)
                                 for x in (jnp.where(mask, p[i:i + W], 0.0), p[i + W:i + step])[:step // W]], axis=0)
        ds = p * (dot(do, v, 1, 1) - jnp.concatenate([delta] * n, axis=1))
        return p.astype(BF16), ds.astype(BF16)

    def chunk_step(g):
        cols = pl.ds(g * W, W)
        k, v = kv[0, cols, :], kv[1, cols, :]
        blocks = [pl.ds(h * T, 2 * T) for h in range(0, G, 2)]
        done = [scores(q_v[rows, :], do_v[rows, :], k, v, lcol[rows, :], dcol[rows, :]) for rows in blocks]
        for rows, (p, ds) in zip(blocks, done):
            dq[rows, :] += dot(ds, k, 1, 0)
            acc[g, 0] += dot(q_v[rows, :], ds, 0, 0)
            acc[g, 1] += dot(do_v[rows, :], p, 0, 0)

    def pair_step(heads):
        row0 = (1 - odd) * (G * T)
        g0 = 2 * even_dev
        lse_t = jnp.transpose(lse_v[1, :, :] * LOG2E)
        k, v = kv[0, even_rows, :], kv[1, even_rows, :]
        blocks = [pl.ds(pl.multiple_of(row0 + h * T, T), T) for h in heads]
        for h, rows in zip(heads, blocks):
            rows_setup(lse_t, 3 + h, rows)
        done = [scores(q_v[rows, :], do_v[rows, :], k, v, lcol[rows, :], dcol[rows, :]) for rows in blocks]
        for rows, (p, ds) in zip(blocks, done):
            dq[rows, :] += dot(ds, k, 1, 0)
            dk = dot(q_v[rows, :], ds, 0, 0)
            dv = dot(do_v[rows, :], p, 0, 0)
            for c in range(2):
                acc[g0 + c, 0] += dk[:, c * W:(c + 1) * W]
                acc[g0 + c, 1] += dv[:, c * W:(c + 1) * W]

    def diag_step(heads, setup_heads):
        g0 = 2 * me
        k, v = kv[0, mine, :], kv[1, mine, :]
        row_i = lax.broadcasted_iota(jnp.int32, (W, W), 0)
        col_i = lax.broadcasted_iota(jnp.int32, (W, W), 1)
        mask = col_i <= row_i
        if setup_heads:
            lse_t = jnp.transpose(lse_v[0, :, :] * LOG2E)

        def low(x):
            return jnp.concatenate([x[W:T], x[T + W:]], axis=0)

        for h in heads:
            if setup_heads:
                for i in range(2):
                    rows_setup(lse_t, h + i, pl.ds((h + i) * T, T))
            rows = pl.ds(h * T, 2 * T)
            lse_col, delta = lcol[rows, :], dcol[rows, :]
            q, do = q_v[rows, :], do_v[rows, :]
            p0, ds0 = scores(q, do, k[:W], v[:W], lse_col, delta, mask)
            q1, do1 = low(q), low(do)
            p1, ds1 = scores(q1, do1, k[W:], v[W:], low(lse_col), low(delta), mask)
            dq0, dq1 = dot(ds0, k[:W], 1, 0), dot(ds1, k[W:], 1, 0)
            new = [x for i in range(2) for x in (dq0[i * T:i * T + W], dq0[i * T + W:(i + 1) * T] + dq1[i * W:(i + 1) * W])]
            if h < 4:
                dq[rows, :] = jnp.concatenate(new, axis=0)
            else:
                dq[rows, :] += jnp.concatenate(new, axis=0)
            acc[g0, 0] += dot(q, ds0, 0, 0)
            acc[g0, 1] += dot(do, p0, 0, 0)
            acc[g0 + 1, 0] += dot(q1, ds1, 0, 0)
            acc[g0 + 1, 1] += dot(do1, p1, 0, 0)
        for h in range(max(heads) + 2, setup_heads):
            rows_setup(lse_t, h, pl.ds(h * T, T))

    def return_chunk(g):
        if g == 0:
            for n in range(2):
                first_sum[n].wait_recv()
                acc[0, n] += cr[0, n]
                first_back[n].start()
            return
        chip_sum[g].wait_recv()
        if g == 1:
            acc[g] += cr[g]
        else:
            part[g - 2].wait_recv()
            total = acc[g] + cr[g] + pr[g - 2]
            fs[g - 2, 0] = (total[0] * SCALE).astype(BF16)
            fs[g - 2, 1] = total[1].astype(BF16)
            (first_sum[0] if g == 2 else chip_sum[1]).wait_send()
        back[g].start()

    with scope('diag_a'):
        diag_step((0, 2), G)

    with scope('go'):
        when(me != 3, lambda: pl.semaphore_wait(go, 1))

    when(odd == 0, kv_pair.start)
    when(me == 1, moved[0].start, moved[1].start)

    with scope('diag_b'):
        when(me != 3, lambda: diag_step((4,), 0))

    when(me == 1, kv_x[2].start, kv_x[3].start, part[0].start, part[1].start)

    def forward(g):
        kv_x[g].wait_recv()
        if g >= 2:
            kv_f[g - 2].wait_send()
        kv_f[g].start()

    @pl.when(chip == 1)
    def _():
        with scope('wait_x'):
            when(odd == 1, lambda: forward(0), moved[0].start, moved[1].start)
        for g in range(4):
            with scope('wait_f'):
                when(odd == 0, kv_f[g].wait_recv)
            with scope('cross'):
                chunk_step(g)
            with scope('sum'):
                if g < 2:
                    when(odd == 1, *(cp.start for cp in (chip_sum[1:2] if g else first_sum)), lambda: forward(g + 1))
                    when(odd == 0, lambda: return_chunk(g))
                else:
                    when(odd == 0, chip_sum[g].start)
            if g == 1:
                with scope('diag_b'):
                    @pl.when(odd == 1)
                    def _():
                        diag_step((4,), 0)
                        forward(3)

        with scope('return2'):
            when(odd == 1, lambda: return_chunk(2))

    with scope('wait_pair'):
        when(odd == 0, moved[0].wait_recv, moved[1].wait_recv)

        @pl.when(odd == 1)
        def _():
            lse_v[1, 3:6, :] = lse_v[0, 0:3, :]
            kv_pair.wait_recv()

    with scope('pair'):
        pair_step((0,))

    with scope('return3'):
        when(me == 3, lambda: return_chunk(3))

    with scope('pair'):
        pair_step((1, 2))

    when(odd == 0, dq_back.start)
    when(odd == 1, local_back.start)

    with scope('results'):
        @pl.when(odd == 1)
        def _():
            dq_back.wait_recv()
            dq[HALF, :] += dqr[...]

        gq_ref[...] = (dq[0:G * T, :] * SCALE).astype(BF16)

        @pl.when(odd == 0)
        def _():
            local_back.wait_recv()
            acc[own] += lr[...]

        @pl.when(me == 0)
        def _():
            for cp in first_back + back[1:2]:
                cp.wait_recv()
            acc[own] += fr[...]

        @pl.when(me == 1)
        def _():
            for c in range(2):
                back[2 + c].wait_recv()
                gk_ref[c * W:(c + 1) * W, :] = jnp.transpose(fb[c, 0])
                gv_ref[c * W:(c + 1) * W, :] = jnp.transpose(fb[c, 1])

        @pl.when(me != 1)
        def _():
            for c in range(2):
                gk_ref[c * W:(c + 1) * W, :] = jnp.transpose(acc[2 * me + c, 0] * SCALE).astype(BF16)
                gv_ref[c * W:(c + 1) * W, :] = jnp.transpose(acc[2 * me + c, 1]).astype(BF16)

    with scope('sends'):
        when(odd == 0, kv_pair.wait_send, dq_back.wait_send)
        when(odd == 1, moved[0].wait_send, moved[1].wait_send, local_back.wait_send)
        when(me == 0, kv_x[0].wait_send, kv_x[1].wait_send)
        when(me == 1, kv_x[2].wait_send, kv_x[3].wait_send, part[0].wait_send, part[1].wait_send)
        when(me == 2, *(cp.wait_send for cp in first_back + back[1:2] + chip_sum[2:]))
        when(me == 3, *(cp.wait_send for cp in kv_f[2:] + first_sum[1:] + back[2:]))


def write_out(gq_v, gk_v, gv_v, gq_hbm, gk_hbm, gv_hbm, sem):
    pairs = [(gq_v, gq_hbm), (gk_v, gk_hbm), (gv_v, gv_hbm)]
    copies = [pltpu.make_async_copy(a, b, sem.at[i]) for i, (a, b) in enumerate(pairs)]
    for cp in copies:
        cp.start()
    for cp in copies:
        cp.wait()


def solution(mesh):
    row_spec = P(('dp', 'cp'))
    vmem = pl.BlockSpec(memory_space=pltpu.VMEM)
    hbm = pl.BlockSpec(memory_space=pltpu.HBM)
    ext = G * T * 3 // 2

    def local_fn(q_tok, k_tok, v_tok, fwd_out, d_out, lse_row):
        def flat(x):
            return jnp.transpose(x, (1, 0, 2)).reshape(G * T, E)

        results = (jax.ShapeDtypeStruct((G * T, E), BF16), jax.ShapeDtypeStruct((T, E), BF16), jax.ShapeDtypeStruct((T, E), BF16))
        staged = pl.pallas_call(
            kernel,
            out_shape=results,
            in_specs=[hbm] * 6,
            out_specs=(vmem, vmem, vmem),
            scratch_shapes=[
                pltpu.VMEM((3, ext, E), BF16), pltpu.VMEM((2, G, T), F32), pltpu.VMEM((ext, E), F32), pltpu.VMEM((ext, E), F32),
                pltpu.VMEM((2, 4 * T, E), BF16), pltpu.VMEM((8, 2, E, W), F32), pltpu.VMEM((ext, E), F32),
                pltpu.VMEM((G * T // 2, E), F32), pltpu.VMEM((2, 2, E, W), F32), pltpu.VMEM((4, 2, E, W), F32),
                pltpu.VMEM((2, 2, E, W), F32), pltpu.VMEM((2, 2, E, W), F32),
                pltpu.VMEM((2, 2, E, W), BF16), pltpu.VMEM((2, 2, E, W), BF16),
                pltpu.SemaphoreType.DMA((6,)), pltpu.SemaphoreType.DMA((8,)), pltpu.SemaphoreType.DMA((10,)), pltpu.SemaphoreType.REGULAR,
            ],
            compiler_params=pltpu.CompilerParams(collective_id=0, has_side_effects=True, vmem_limit_bytes=40 * 2 ** 20),
            name='attention_backward',
        )(*[pltpu.with_memory_space_constraint(x, pltpu.HBM) for x in (flat(q_tok), k_tok, v_tok, flat(fwd_out), flat(d_out), lse_row.T)])
        gq, gk, gv = pl.pallas_call(
            write_out,
            out_shape=results,
            in_specs=[vmem] * 3,
            out_specs=(hbm,) * 3,
            scratch_shapes=[pltpu.SemaphoreType.DMA((3,))],
            compiler_params=pltpu.CompilerParams(vmem_limit_bytes=4 * 2 ** 20),
            name='write_out',
        )(*staged)
        return jnp.transpose(gq.reshape(G, T, E), (1, 0, 2)), gk, gv

    return jax.shard_map(local_fn, mesh=mesh, in_specs=(row_spec,) * 6, out_specs=(row_spec,) * 3, check_vma=False)
```

```python
import functools

import jax
import jax.numpy as jnp
from jax import lax
from jax.experimental import pallas as pl
from jax.experimental.pallas import tpu as pltpu
from jax.sharding import PartitionSpec as P

F32 = jnp.float32
BF16 = jnp.bfloat16
MESH = pl.DeviceIdType.MESH
T = 512
G = 6
E = 128
W = 256
SCALE = E ** -0.5
LOG2E = 1.4426950408889634


def dot(a, b, ca, cb):
    return lax.dot_general(a, b, (((ca,), (cb,)), ((), ())), preferred_element_type=F32)


def kernel(q_hbm, k_hbm, v_hbm, o_hbm, do_hbm, lse_hbm, gq_ref, gk_ref, gv_ref,
           x_v, lse_v, lcol, dcol, kv, acc, dq, dqr, lr, cr, pr, fr, fs, fb, ss, rs, go):
    dp = lax.axis_index('dp')
    me = lax.axis_index('cp')
    chip = me // 2
    odd = me - 2 * chip
    even_dev = 2 * chip
    odd_dev = 2 * chip + 1
    scope = jax.named_scope
    do_v, o_v, q_v = x_v.at[0], x_v.at[1], x_v.at[2]

    def rcopy(i, j, src, dst, dev):
        return pltpu.make_async_remote_copy(src, dst, ss.at[i], rs.at[j], device_id=(dp, dev), device_id_type=MESH)

    def when(cond, *fns):
        @pl.when(cond)
        def _():
            for f in fns:
                f()

    mine = pl.ds(me * T, T)
    loads = [pltpu.make_async_copy(src, dst, ss.at[n]) for n, (src, dst) in enumerate((
        (k_hbm, kv.at[0, mine]), (v_hbm, kv.at[1, mine]), (lse_hbm, lse_v.at[0]),
        (do_hbm, do_v.at[pl.ds(0, G * T)]), (o_hbm, o_v.at[pl.ds(0, G * T)]), (q_hbm, q_v.at[pl.ds(0, G * T)])))]
    for cp in loads:
        cp.start()

    bar = pltpu.get_barrier_semaphore()

    def greet(sem, dev):
        pl.semaphore_signal(sem, 1, device_id=(dp, dev), device_id_type=MESH)

    @pl.when(me == 3)
    def _():
        for d in range(3):
            greet(bar, d)

    when(me != 3, lambda: greet(bar, 3))
    with scope('barrier'):
        when(me == 3, lambda: pl.semaphore_wait(bar, 3))
        when(me != 3, lambda: pl.semaphore_wait(bar, 1))

    @pl.when(me == 3)
    def _():
        for d in range(3):
            greet(go, d)

    own = pl.ds(2 * me, 2)
    HALF = pl.ds(G * T // 2, G * T // 2)
    MOVED = pl.ds(G * T, G * T // 2)
    even_rows = pl.ds(even_dev * T, T)

    def kv_chunk(g):
        return kv.at[:, pl.ds(g * W, W)]

    kv_pair = rcopy(2, 0, kv.at[:, even_rows], kv.at[:, even_rows], odd_dev)
    dq_back = rcopy(3, 1, dq.at[MOVED], dqr, odd_dev)
    moved = [rcopy(0, 0, lse_v.at[0], lse_v.at[1], even_dev), rcopy(1, 1, x_v.at[:, HALF], x_v.at[:, MOVED], even_dev)]
    local_back = rcopy(2, 2, acc.at[pl.ds(2 * even_dev, 2)], lr, even_dev)
    kv_x = [rcopy((0, 1, 3, 4)[g], 2 + g, kv_chunk(g), kv_chunk(g), 3) for g in range(4)]
    kv_f = [rcopy(3 + g % 2, 3 + g, kv_chunk(g), kv_chunk(g), 2) for g in range(4)]
    sum0 = [rcopy(5 + n, 7 + n, acc.at[0, n], cr.at[0, n], 2) for n in range(2)]
    sum1 = rcopy(7, 9, acc.at[1], cr.at[1], 2)
    sum2 = rcopy(5, 6, acc.at[2], cr.at[2], 3)
    sum3 = [rcopy(6 + n, 7 + n, acc.at[3, n], cr.at[3, n], 3) for n in range(2)]
    part = [rcopy(5 + c, 9 + c, acc.at[2 + c], pr.at[c], 3) for c in range(2)]
    back0 = [rcopy(n, 3 + n, acc.at[0, n], fr.at[0, n], 0) for n in range(2)]
    back1 = rcopy(4, 5, acc.at[1], fr.at[1], 0)
    back2 = rcopy(5, 2, fs.at[0], fb.at[0], 1)
    back3 = [rcopy(6 + n, 3 + n, fs.at[1, n], fb.at[1, n], 1) for n in range(2)]

    with scope('wait_kv'):
        loads[0].wait()
        loads[1].wait()

    when(me == 0, kv_x[0].start, kv_x[1].start)

    with scope('zero_wait_loads'):
        acc[...] = jnp.zeros_like(acc)
        zeros = pl.ds(4 * T, (G - 4) * T + G * T // 2)
        dq[zeros, :] = jnp.zeros((zeros.size, E), F32)
        for cp in loads[2:]:
            cp.wait()

    def rows_setup(lse_t, head, rows):
        lcol[rows, :] = jnp.broadcast_to(lse_t[:, head:head + 1], (T, E))
        delta = jnp.sum(do_v[rows, :].astype(F32) * o_v[rows, :].astype(F32), axis=1, keepdims=True)
        dcol[rows, :] = jnp.broadcast_to(delta, (T, E))

    def scores(q, do, k, v, lse_col, delta, mask=None):
        n = k.shape[0] // E
        p = jnp.exp2(dot(q, k, 1, 1) * (SCALE * LOG2E) - jnp.concatenate([lse_col] * n, axis=1))
        if mask is not None:
            step = p.shape[0] // 2
            p = jnp.concatenate([x for i in range(0, 2 * step, step)
                                 for x in (jnp.where(mask, p[i:i + W], 0.0), p[i + W:i + step])[:step // W]], axis=0)
        ds = p * (dot(do, v, 1, 1) - jnp.concatenate([delta] * n, axis=1))
        return p.astype(BF16), ds.astype(BF16)

    def chunk_step(g):
        cols = pl.ds(g * W, W)
        k, v = kv[0, cols, :], kv[1, cols, :]
        blocks = [pl.ds(h * T, 2 * T) for h in range(0, G, 2)]
        done = [scores(q_v[rows, :], do_v[rows, :], k, v, lcol[rows, :], dcol[rows, :]) for rows in blocks]
        for rows, (p, ds) in zip(blocks, done):
            dq[rows, :] += dot(ds, k, 1, 0)
            acc[g, 0] += dot(q_v[rows, :], ds, 0, 0)
            acc[g, 1] += dot(do_v[rows, :], p, 0, 0)

    def pair_step(heads):
        row0 = (1 - odd) * (G * T)
        g0 = 2 * even_dev
        lse_t = jnp.transpose(lse_v[1, :, :] * LOG2E)
        k, v = kv[0, even_rows, :], kv[1, even_rows, :]
        blocks = [pl.ds(pl.multiple_of(row0 + h * T, T), T) for h in heads]
        for h, rows in zip(heads, blocks):
            rows_setup(lse_t, 3 + h, rows)
        done = [scores(q_v[rows, :], do_v[rows, :], k, v, lcol[rows, :], dcol[rows, :]) for rows in blocks]
        for rows, (p, ds) in zip(blocks, done):
            dq[rows, :] += dot(ds, k, 1, 0)
            dk = dot(q_v[rows, :], ds, 0, 0)
            dv = dot(do_v[rows, :], p, 0, 0)
            for c in range(2):
                acc[g0 + c, 0] += dk[:, c * W:(c + 1) * W]
                acc[g0 + c, 1] += dv[:, c * W:(c + 1) * W]

    def diag_step(heads, setup_heads):
        g0 = 2 * me
        k, v = kv[0, mine, :], kv[1, mine, :]
        row_i = lax.broadcasted_iota(jnp.int32, (W, W), 0)
        col_i = lax.broadcasted_iota(jnp.int32, (W, W), 1)
        mask = col_i <= row_i
        if setup_heads:
            lse_t = jnp.transpose(lse_v[0, :, :] * LOG2E)

        def low(x):
            return jnp.concatenate([x[W:T], x[T + W:]], axis=0)

        for h in heads:
            if setup_heads:
                for i in range(2):
                    rows_setup(lse_t, h + i, pl.ds((h + i) * T, T))
            rows = pl.ds(h * T, 2 * T)
            lse_col, delta = lcol[rows, :], dcol[rows, :]
            q, do = q_v[rows, :], do_v[rows, :]
            p0, ds0 = scores(q, do, k[:W], v[:W], lse_col, delta, mask)
            q1, do1 = low(q), low(do)
            p1, ds1 = scores(q1, do1, k[W:], v[W:], low(lse_col), low(delta), mask)
            dq0, dq1 = dot(ds0, k[:W], 1, 0), dot(ds1, k[W:], 1, 0)
            new = [x for i in range(2) for x in (dq0[i * T:i * T + W], dq0[i * T + W:(i + 1) * T] + dq1[i * W:(i + 1) * W])]
            if h < 4:
                dq[rows, :] = jnp.concatenate(new, axis=0)
            else:
                dq[rows, :] += jnp.concatenate(new, axis=0)
            acc[g0, 0] += dot(q, ds0, 0, 0)
            acc[g0, 1] += dot(do, p0, 0, 0)
            acc[g0 + 1, 0] += dot(q1, ds1, 0, 0)
            acc[g0 + 1, 1] += dot(do1, p1, 0, 0)
        for h in range(max(heads) + 2, setup_heads):
            rows_setup(lse_t, h, pl.ds(h * T, T))

    def return_chunk(g):
        if g == 0:
            for n in range(2):
                sum0[n].wait_recv()
                acc[0, n] += cr[0, n]
                back0[n].start()
        elif g == 1:
            sum1.wait_recv()
            acc[1] += cr[1]
            back1.start()
        elif g == 2:
            sum2.wait_recv()
            part[0].wait_recv()
            total = acc[2] + cr[2] + pr[0]
            fs[0, 0] = (total[0] * SCALE).astype(BF16)
            fs[0, 1] = total[1].astype(BF16)
            sum0[0].wait_send()
            back2.start()
        else:
            part[1].wait_recv()
            sum0[1].wait_send()
            sum1.wait_send()
            for n in range(2):
                sum3[n].wait_recv()
                total = acc[3, n] + cr[3, n] + pr[1, n]
                fs[1, n] = (total * SCALE if n == 0 else total).astype(BF16)
                back3[n].start()

    with scope('diag_a'):
        diag_step((0, 2), G)

    with scope('go'):
        when(me != 3, lambda: pl.semaphore_wait(go, 1))

    when(odd == 0, kv_pair.start)
    when(me == 1, moved[0].start, moved[1].start)

    with scope('diag_b'):
        when(me != 3, lambda: diag_step((4,), 0))

    when(me == 1, kv_x[2].start, kv_x[3].start, part[0].start, part[1].start)

    def forward(g):
        kv_x[g].wait_recv()
        if g >= 2:
            kv_f[g - 2].wait_send()
        kv_f[g].start()

    @pl.when(chip == 1)
    def _():
        with scope('wait_x'):
            when(odd == 1, lambda: forward(0), moved[0].start, moved[1].start)
        for g in range(4):
            with scope('wait_f'):
                when(odd == 0, kv_f[g].wait_recv)
            with scope('cross'):
                chunk_step(g)
            with scope('sum'):
                if g < 2:
                    when(odd == 1, *(cp.start for cp in ([sum1] if g else sum0)), lambda: forward(g + 1))
                    when(odd == 0, lambda: return_chunk(g))
                else:
                    when(odd == 0, *(cp.start for cp in ([sum2] if g == 2 else sum3)))
            if g == 1:
                with scope('diag_b'):
                    @pl.when(odd == 1)
                    def _():
                        diag_step((4,), 0)
                        forward(3)

        with scope('return2'):
            when(odd == 1, lambda: return_chunk(2))

    with scope('wait_pair'):
        when(odd == 0, moved[0].wait_recv, moved[1].wait_recv)

        @pl.when(odd == 1)
        def _():
            lse_v[1, 3:6, :] = lse_v[0, 0:3, :]
            kv_pair.wait_recv()

    with scope('pair'):
        pair_step((0,))

    with scope('return3'):
        when(me == 3, lambda: return_chunk(3))

    with scope('pair'):
        pair_step((1, 2))

    when(odd == 0, dq_back.start)
    when(odd == 1, local_back.start)

    with scope('results'):
        @pl.when(odd == 1)
        def _():
            dq_back.wait_recv()
            dq[HALF, :] += dqr[...]

        gq_ref[...] = (dq[0:G * T, :] * SCALE).astype(BF16)

        @pl.when(odd == 0)
        def _():
            local_back.wait_recv()
            acc[own] += lr[...]

        @pl.when(me == 0)
        def _():
            for cp in back0 + [back1]:
                cp.wait_recv()
            acc[own] += fr[...]

        @pl.when(me == 1)
        def _():
            back2.wait_recv()
            gk_ref[0:W, :] = jnp.transpose(fb[0, 0])
            gv_ref[0:W, :] = jnp.transpose(fb[0, 1])
            back3[0].wait_recv()
            gk_ref[W:T, :] = jnp.transpose(fb[1, 0])
            back3[1].wait_recv()
            gv_ref[W:T, :] = jnp.transpose(fb[1, 1])

        @pl.when(me != 1)
        def _():
            for c in range(2):
                gk_ref[c * W:(c + 1) * W, :] = jnp.transpose(acc[2 * me + c, 0] * SCALE).astype(BF16)
                gv_ref[c * W:(c + 1) * W, :] = jnp.transpose(acc[2 * me + c, 1]).astype(BF16)

    with scope('sends'):
        when(odd == 0, kv_pair.wait_send, dq_back.wait_send)
        when(odd == 1, moved[0].wait_send, moved[1].wait_send, local_back.wait_send)
        when(me == 0, kv_x[0].wait_send, kv_x[1].wait_send)
        when(me == 1, kv_x[2].wait_send, kv_x[3].wait_send, part[0].wait_send, part[1].wait_send)
        when(me == 2, *(cp.wait_send for cp in back0 + [back1, sum2] + sum3))
        when(me == 3, *(cp.wait_send for cp in kv_f[2:] + [back2] + back3))


def write_out(gq_v, gk_v, gv_v, gq_hbm, gk_hbm, gv_hbm, sem):
    pairs = [(gq_v, gq_hbm), (gk_v, gk_hbm), (gv_v, gv_hbm)]
    copies = [pltpu.make_async_copy(a, b, sem.at[i]) for i, (a, b) in enumerate(pairs)]
    for cp in copies:
        cp.start()
    for cp in copies:
        cp.wait()


def solution(mesh):
    row_spec = P(('dp', 'cp'))
    vmem = pl.BlockSpec(memory_space=pltpu.VMEM)
    hbm = pl.BlockSpec(memory_space=pltpu.HBM)
    ext = G * T * 3 // 2

    def local_fn(q_tok, k_tok, v_tok, fwd_out, d_out, lse_row):
        def flat(x):
            return jnp.transpose(x, (1, 0, 2)).reshape(G * T, E)

        results = (jax.ShapeDtypeStruct((G * T, E), BF16), jax.ShapeDtypeStruct((T, E), BF16), jax.ShapeDtypeStruct((T, E), BF16))
        staged = pl.pallas_call(
            kernel,
            out_shape=results,
            in_specs=[hbm] * 6,
            out_specs=(vmem, vmem, vmem),
            scratch_shapes=[
                pltpu.VMEM((3, ext, E), BF16), pltpu.VMEM((2, G, T), F32), pltpu.VMEM((ext, E), F32), pltpu.VMEM((ext, E), F32),
                pltpu.VMEM((2, 4 * T, E), BF16), pltpu.VMEM((8, 2, E, W), F32), pltpu.VMEM((ext, E), F32),
                pltpu.VMEM((G * T // 2, E), F32), pltpu.VMEM((2, 2, E, W), F32), pltpu.VMEM((4, 2, E, W), F32),
                pltpu.VMEM((2, 2, E, W), F32), pltpu.VMEM((2, 2, E, W), F32),
                pltpu.VMEM((2, 2, E, W), BF16), pltpu.VMEM((2, 2, E, W), BF16),
                pltpu.SemaphoreType.DMA((8,)), pltpu.SemaphoreType.DMA((11,)), pltpu.SemaphoreType.REGULAR,
            ],
            compiler_params=pltpu.CompilerParams(collective_id=0, has_side_effects=True, vmem_limit_bytes=40 * 2 ** 20),
            name='attention_backward',
        )(*[pltpu.with_memory_space_constraint(x, pltpu.HBM) for x in (flat(q_tok), k_tok, v_tok, flat(fwd_out), flat(d_out), lse_row.T)])
        gq, gk, gv = pl.pallas_call(
            write_out,
            out_shape=results,
            in_specs=[vmem] * 3,
            out_specs=(hbm,) * 3,
            scratch_shapes=[pltpu.SemaphoreType.DMA((3,))],
            compiler_params=pltpu.CompilerParams(vmem_limit_bytes=4 * 2 ** 20),
            name='write_out',
        )(*staged)
        return jnp.transpose(gq.reshape(G, T, E), (1, 0, 2)), gk, gv

    return jax.shard_map(local_fn, mesh=mesh, in_specs=(row_spec,) * 6, out_specs=(row_spec,) * 3, check_vma=False)
```

```python
import functools

import jax
import jax.numpy as jnp
from jax import lax
from jax.experimental import pallas as pl
from jax.experimental.pallas import tpu as pltpu
from jax.sharding import PartitionSpec as P

F32 = jnp.float32
BF16 = jnp.bfloat16
MESH = pl.DeviceIdType.MESH
T = 512
G = 6
E = 128
W = 256
SCALE = E ** -0.5
LOG2E = 1.4426950408889634


def dot(a, b, ca, cb):
    return lax.dot_general(a, b, (((ca,), (cb,)), ((), ())), preferred_element_type=F32)


def kernel(q_hbm, k_hbm, v_hbm, o_hbm, do_hbm, lse_hbm, gq_ref, gk_ref, gv_ref,
           x_v, lse_v, lcol, dcol, kv, acc, dq, dqr, lr, cr, pr, fr, fs, fb, ss, rs, go):
    dp = lax.axis_index('dp')
    me = lax.axis_index('cp')
    chip = me // 2
    odd = me - 2 * chip
    even_dev = 2 * chip
    odd_dev = 2 * chip + 1
    scope = jax.named_scope
    do_v, o_v, q_v = x_v.at[0], x_v.at[1], x_v.at[2]

    def rcopy(i, j, src, dst, dev):
        return pltpu.make_async_remote_copy(src, dst, ss.at[i], rs.at[j], device_id=(dp, dev), device_id_type=MESH)

    def when(cond, *fns):
        @pl.when(cond)
        def _():
            for f in fns:
                f()

    mine = pl.ds(me * T, T)
    loads = [pltpu.make_async_copy(src, dst, ss.at[n]) for n, (src, dst) in enumerate((
        (k_hbm, kv.at[0, mine]), (v_hbm, kv.at[1, mine]), (lse_hbm, lse_v.at[0]),
        (do_hbm, do_v.at[pl.ds(0, G * T)]), (o_hbm, o_v.at[pl.ds(0, G * T)]), (q_hbm, q_v.at[pl.ds(0, G * T)])))]
    for cp in loads:
        cp.start()

    bar = pltpu.get_barrier_semaphore()

    def greet(sem, dev):
        pl.semaphore_signal(sem, 1, device_id=(dp, dev), device_id_type=MESH)

    @pl.when(me == 3)
    def _():
        for d in range(3):
            greet(bar, d)

    when(me != 3, lambda: greet(bar, 3))
    with scope('barrier'):
        when(me == 3, lambda: pl.semaphore_wait(bar, 3))
        when(me != 3, lambda: pl.semaphore_wait(bar, 1))

    @pl.when(me == 3)
    def _():
        for d in range(3):
            greet(go, d)

    own = pl.ds(2 * me, 2)
    HALF = pl.ds(G * T // 2, G * T // 2)
    MOVED = pl.ds(G * T, G * T // 2)
    even_rows = pl.ds(even_dev * T, T)

    def kv_chunk(g):
        return kv.at[:, pl.ds(g * W, W)]

    kv_pair = rcopy(2, 0, kv.at[:, even_rows], kv.at[:, even_rows], odd_dev)
    dq_back = rcopy(3, 1, dq.at[MOVED], dqr, odd_dev)
    moved = [rcopy(0, 0, lse_v.at[0], lse_v.at[1], even_dev), rcopy(1, 1, x_v.at[:, HALF], x_v.at[:, MOVED], even_dev)]
    local_back = rcopy(2, 2, acc.at[pl.ds(2 * even_dev, 2)], lr, even_dev)
    kv_x = [rcopy((0, 1, 3, 4)[g], 2 + g, kv_chunk(g), kv_chunk(g), 3) for g in range(4)]
    kv_f = [rcopy(3 + g % 2, 3 + g, kv_chunk(g), kv_chunk(g), 2) for g in range(4)]
    sum0 = [rcopy(5 + n, 7 + n, acc.at[0, n], cr.at[0, n], 2) for n in range(2)]
    sum1 = rcopy(7, 9, acc.at[1], cr.at[1], 2)
    sum2 = rcopy(5, 6, acc.at[2], cr.at[2], 3)
    sum3 = [rcopy(6 + n, 7 + n, acc.at[3, n], cr.at[3, n], 3) for n in range(2)]
    part = [rcopy(5 + c, 9 + c, acc.at[2 + c], pr.at[c], 3) for c in range(2)]
    back0 = [rcopy(n, 3 + n, acc.at[0, n], fr.at[0, n], 0) for n in range(2)]
    back1 = rcopy(4, 5, acc.at[1], fr.at[1], 0)
    back2 = rcopy(5, 2, fs.at[0], fb.at[0], 1)
    back3 = [rcopy(6 + n, 3 + n, fs.at[1, n], fb.at[1, n], 1) for n in range(2)]

    with scope('wait_kv'):
        loads[0].wait()
        loads[1].wait()

    when(me == 0, kv_x[0].start, kv_x[1].start)

    with scope('zero_wait_loads'):
        @pl.loop(0, 8)
        def _(g):
            acc[g] = jnp.zeros((2, E, W), F32)

        @pl.loop(4, G + 3)
        def _(h):
            dq[pl.ds(pl.multiple_of(h * T, T), T), :] = jnp.zeros((T, E), F32)

        for cp in loads[2:]:
            cp.wait()

    def rows_setup(lse_t, head, rows):
        lcol[rows, :] = jnp.broadcast_to(lse_t[:, head:head + 1], (T, E))
        delta = jnp.sum(do_v[rows, :].astype(F32) * o_v[rows, :].astype(F32), axis=1, keepdims=True)
        dcol[rows, :] = jnp.broadcast_to(delta, (T, E))

    def scores(q, do, k, v, lse_col, delta, mask=None):
        n = k.shape[0] // E
        p = jnp.exp2(dot(q, k, 1, 1) * (SCALE * LOG2E) - jnp.concatenate([lse_col] * n, axis=1))
        if mask is not None:
            step = p.shape[0] // 2
            p = jnp.concatenate([x for i in range(0, 2 * step, step)
                                 for x in (jnp.where(mask, p[i:i + W], 0.0), p[i + W:i + step])[:step // W]], axis=0)
        ds = p * (dot(do, v, 1, 1) - jnp.concatenate([delta] * n, axis=1))
        return p.astype(BF16), ds.astype(BF16)

    def chunk_step(g):
        cols = pl.ds(g * W, W)
        k, v = kv[0, cols, :], kv[1, cols, :]
        blocks = [pl.ds(h * T, 2 * T) for h in range(0, G, 2)]
        done = [scores(q_v[rows, :], do_v[rows, :], k, v, lcol[rows, :], dcol[rows, :]) for rows in blocks]
        for rows, (p, ds) in zip(blocks, done):
            dq[rows, :] += dot(ds, k, 1, 0)
            acc[g, 0] += dot(q_v[rows, :], ds, 0, 0)
            acc[g, 1] += dot(do_v[rows, :], p, 0, 0)

    def pair_step(heads):
        row0 = (1 - odd) * (G * T)
        g0 = 2 * even_dev
        lse_t = jnp.transpose(lse_v[1, :, :] * LOG2E)
        k, v = kv[0, even_rows, :], kv[1, even_rows, :]
        blocks = [pl.ds(pl.multiple_of(row0 + h * T, T), T) for h in heads]
        for h, rows in zip(heads, blocks):
            rows_setup(lse_t, 3 + h, rows)
        done = [scores(q_v[rows, :], do_v[rows, :], k, v, lcol[rows, :], dcol[rows, :]) for rows in blocks]
        for rows, (p, ds) in zip(blocks, done):
            dq[rows, :] += dot(ds, k, 1, 0)
            dk = dot(q_v[rows, :], ds, 0, 0)
            dv = dot(do_v[rows, :], p, 0, 0)
            for c in range(2):
                acc[g0 + c, 0] += dk[:, c * W:(c + 1) * W]
                acc[g0 + c, 1] += dv[:, c * W:(c + 1) * W]

    def diag_step(heads, setup_heads):
        g0 = 2 * me
        k, v = kv[0, mine, :], kv[1, mine, :]
        row_i = lax.broadcasted_iota(jnp.int32, (W, W), 0)
        col_i = lax.broadcasted_iota(jnp.int32, (W, W), 1)
        mask = col_i <= row_i
        if setup_heads:
            lse_t = jnp.transpose(lse_v[0, :, :] * LOG2E)

        def low(x):
            return jnp.concatenate([x[W:T], x[T + W:]], axis=0)

        for h in heads:
            if setup_heads:
                for i in range(2):
                    rows_setup(lse_t, h + i, pl.ds((h + i) * T, T))
            rows = pl.ds(h * T, 2 * T)
            lse_col, delta = lcol[rows, :], dcol[rows, :]
            q, do = q_v[rows, :], do_v[rows, :]
            p0, ds0 = scores(q, do, k[:W], v[:W], lse_col, delta, mask)
            q1, do1 = low(q), low(do)
            p1, ds1 = scores(q1, do1, k[W:], v[W:], low(lse_col), low(delta), mask)
            dq0, dq1 = dot(ds0, k[:W], 1, 0), dot(ds1, k[W:], 1, 0)
            new = [x for i in range(2) for x in (dq0[i * T:i * T + W], dq0[i * T + W:(i + 1) * T] + dq1[i * W:(i + 1) * W])]
            if h < 4:
                dq[rows, :] = jnp.concatenate(new, axis=0)
            else:
                dq[rows, :] += jnp.concatenate(new, axis=0)
            acc[g0, 0] += dot(q, ds0, 0, 0)
            acc[g0, 1] += dot(do, p0, 0, 0)
            acc[g0 + 1, 0] += dot(q1, ds1, 0, 0)
            acc[g0 + 1, 1] += dot(do1, p1, 0, 0)
        for h in range(max(heads) + 2, setup_heads):
            rows_setup(lse_t, h, pl.ds(h * T, T))

    def return_chunk(g):
        if g == 0:
            for n in range(2):
                sum0[n].wait_recv()
                acc[0, n] += cr[0, n]
                back0[n].start()
        elif g == 1:
            sum1.wait_recv()
            acc[1] += cr[1]
            back1.start()
        elif g == 2:
            sum2.wait_recv()
            part[0].wait_recv()
            total = acc[2] + cr[2] + pr[0]
            fs[0, 0] = (total[0] * SCALE).astype(BF16)
            fs[0, 1] = total[1].astype(BF16)
            sum0[0].wait_send()
            back2.start()
        else:
            part[1].wait_recv()
            sum0[1].wait_send()
            sum1.wait_send()
            for n in range(2):
                sum3[n].wait_recv()
                total = acc[3, n] + cr[3, n] + pr[1, n]
                fs[1, n] = (total * SCALE if n == 0 else total).astype(BF16)
                back3[n].start()

    with scope('diag_a'):
        diag_step((0, 2), G)

    with scope('go'):
        when(me != 3, lambda: pl.semaphore_wait(go, 1))

    when(odd == 0, kv_pair.start)
    when(me == 1, moved[0].start, moved[1].start)

    with scope('diag_b'):
        when(me != 3, lambda: diag_step((4,), 0))

    when(me == 1, kv_x[2].start, kv_x[3].start, part[0].start, part[1].start)

    def forward(g):
        kv_x[g].wait_recv()
        if g >= 2:
            kv_f[g - 2].wait_send()
        kv_f[g].start()

    @pl.when(chip == 1)
    def _():
        with scope('wait_x'):
            when(odd == 1, lambda: forward(0), moved[0].start, moved[1].start)
        for g in range(4):
            with scope('wait_f'):
                when(odd == 0, kv_f[g].wait_recv)
            with scope('cross'):
                chunk_step(g)
            with scope('sum'):
                if g < 2:
                    when(odd == 1, *(cp.start for cp in ([sum1] if g else sum0)), lambda: forward(g + 1))
                    when(odd == 0, lambda: return_chunk(g))
                else:
                    when(odd == 0, *(cp.start for cp in ([sum2] if g == 2 else sum3)))
            if g == 1:
                with scope('diag_b'):
                    @pl.when(odd == 1)
                    def _():
                        diag_step((4,), 0)
                        forward(3)

        with scope('return2'):
            when(odd == 1, lambda: return_chunk(2))

    with scope('wait_pair'):
        when(odd == 0, moved[0].wait_recv, moved[1].wait_recv)

        @pl.when(odd == 1)
        def _():
            lse_v[1, 3:6, :] = lse_v[0, 0:3, :]
            kv_pair.wait_recv()

    with scope('pair'):
        pair_step((0,))

    with scope('return3'):
        when(me == 3, lambda: return_chunk(3))

    with scope('pair'):
        pair_step((1, 2))

    when(odd == 0, dq_back.start)
    when(odd == 1, local_back.start)

    with scope('results'):
        @pl.when(odd == 1)
        def _():
            dq_back.wait_recv()
            dq[HALF, :] += dqr[...]

        gq_ref[...] = (dq[0:G * T, :] * SCALE).astype(BF16)

        @pl.when(odd == 0)
        def _():
            local_back.wait_recv()
            acc[own] += lr[...]

        @pl.when(me == 0)
        def _():
            for cp in back0 + [back1]:
                cp.wait_recv()
            acc[own] += fr[...]

        @pl.when(me == 1)
        def _():
            back2.wait_recv()
            gk_ref[0:W, :] = jnp.transpose(fb[0, 0])
            gv_ref[0:W, :] = jnp.transpose(fb[0, 1])
            back3[0].wait_recv()
            gk_ref[W:T, :] = jnp.transpose(fb[1, 0])
            back3[1].wait_recv()
            gv_ref[W:T, :] = jnp.transpose(fb[1, 1])

        @pl.when(me != 1)
        def _():
            for c in range(2):
                gk_ref[c * W:(c + 1) * W, :] = jnp.transpose(acc[2 * me + c, 0] * SCALE).astype(BF16)
                gv_ref[c * W:(c + 1) * W, :] = jnp.transpose(acc[2 * me + c, 1]).astype(BF16)

    with scope('sends'):
        when(odd == 0, kv_pair.wait_send, dq_back.wait_send)
        when(odd == 1, moved[0].wait_send, moved[1].wait_send, local_back.wait_send)
        when(me == 0, kv_x[0].wait_send, kv_x[1].wait_send)
        when(me == 1, kv_x[2].wait_send, kv_x[3].wait_send, part[0].wait_send, part[1].wait_send)
        when(me == 2, *(cp.wait_send for cp in back0 + [back1, sum2] + sum3))
        when(me == 3, *(cp.wait_send for cp in kv_f[2:] + [back2] + back3))


def write_out(gq_v, gk_v, gv_v, gq_hbm, gk_hbm, gv_hbm, sem):
    pairs = [(gq_v, gq_hbm), (gk_v, gk_hbm), (gv_v, gv_hbm)]
    copies = [pltpu.make_async_copy(a, b, sem.at[i]) for i, (a, b) in enumerate(pairs)]
    for cp in copies:
        cp.start()
    for cp in copies:
        cp.wait()


def solution(mesh):
    row_spec = P(('dp', 'cp'))
    vmem = pl.BlockSpec(memory_space=pltpu.VMEM)
    hbm = pl.BlockSpec(memory_space=pltpu.HBM)
    ext = G * T * 3 // 2

    def local_fn(q_tok, k_tok, v_tok, fwd_out, d_out, lse_row):
        def flat(x):
            return jnp.transpose(x, (1, 0, 2)).reshape(G * T, E)

        results = (jax.ShapeDtypeStruct((G * T, E), BF16), jax.ShapeDtypeStruct((T, E), BF16), jax.ShapeDtypeStruct((T, E), BF16))
        staged = pl.pallas_call(
            kernel,
            out_shape=results,
            in_specs=[hbm] * 6,
            out_specs=(vmem, vmem, vmem),
            scratch_shapes=[
                pltpu.VMEM((3, ext, E), BF16), pltpu.VMEM((2, G, T), F32), pltpu.VMEM((ext, E), F32), pltpu.VMEM((ext, E), F32),
                pltpu.VMEM((2, 4 * T, E), BF16), pltpu.VMEM((8, 2, E, W), F32), pltpu.VMEM((ext, E), F32),
                pltpu.VMEM((G * T // 2, E), F32), pltpu.VMEM((2, 2, E, W), F32), pltpu.VMEM((4, 2, E, W), F32),
                pltpu.VMEM((2, 2, E, W), F32), pltpu.VMEM((2, 2, E, W), F32),
                pltpu.VMEM((2, 2, E, W), BF16), pltpu.VMEM((2, 2, E, W), BF16),
                pltpu.SemaphoreType.DMA((8,)), pltpu.SemaphoreType.DMA((11,)), pltpu.SemaphoreType.REGULAR,
            ],
            compiler_params=pltpu.CompilerParams(collective_id=0, has_side_effects=True, vmem_limit_bytes=40 * 2 ** 20),
            name='attention_backward',
        )(*[pltpu.with_memory_space_constraint(x, pltpu.HBM) for x in (flat(q_tok), k_tok, v_tok, flat(fwd_out), flat(d_out), lse_row.T)])
        gq, gk, gv = pl.pallas_call(
            write_out,
            out_shape=results,
            in_specs=[vmem] * 3,
            out_specs=(hbm,) * 3,
            scratch_shapes=[pltpu.SemaphoreType.DMA((3,))],
            compiler_params=pltpu.CompilerParams(vmem_limit_bytes=4 * 2 ** 20),
            name='write_out',
        )(*staged)
        return jnp.transpose(gq.reshape(G, T, E), (1, 0, 2)), gk, gv

    return jax.shard_map(local_fn, mesh=mesh, in_specs=(row_spec,) * 6, out_specs=(row_spec,) * 3, check_vma=False)
```

```python
import functools

import jax
import jax.numpy as jnp
from jax import lax
from jax.experimental import pallas as pl
from jax.experimental.pallas import tpu as pltpu
from jax.sharding import PartitionSpec as P

F32 = jnp.float32
BF16 = jnp.bfloat16
MESH = pl.DeviceIdType.MESH
T = 512
G = 6
E = 128
W = 256
SCALE = E ** -0.5
LOG2E = 1.4426950408889634


def dot(a, b, ca, cb):
    return lax.dot_general(a, b, (((ca,), (cb,)), ((), ())), preferred_element_type=F32)


def kernel(q_hbm, k_hbm, v_hbm, o_hbm, do_hbm, lse_hbm, gq_ref, gk_ref, gv_ref,
           x_v, lse_v, lcol, dcol, kv, acc, dq, dqr, lr, cr, pr, fr, fs, fb, ss, rs, go):
    dp = lax.axis_index('dp')
    me = lax.axis_index('cp')
    chip = me // 2
    odd = me - 2 * chip
    even_dev = 2 * chip
    odd_dev = 2 * chip + 1
    scope = jax.named_scope
    do_v, o_v, q_v = x_v.at[0], x_v.at[1], x_v.at[2]

    def rcopy(i, j, src, dst, dev):
        return pltpu.make_async_remote_copy(src, dst, ss.at[i], rs.at[j], device_id=(dp, dev), device_id_type=MESH)

    def when(cond, *fns):
        @pl.when(cond)
        def _():
            for f in fns:
                f()

    mine = pl.ds(me * T, T)
    loads = [pltpu.make_async_copy(src, dst, ss.at[n]) for n, (src, dst) in enumerate((
        (k_hbm, kv.at[0, mine]), (v_hbm, kv.at[1, mine]), (lse_hbm, lse_v.at[0]),
        (do_hbm, do_v.at[pl.ds(0, G * T)]), (o_hbm, o_v.at[pl.ds(0, G * T)]), (q_hbm, q_v.at[pl.ds(0, G * T)])))]
    for cp in loads:
        cp.start()

    bar = pltpu.get_barrier_semaphore()

    def greet(sem, dev):
        pl.semaphore_signal(sem, 1, device_id=(dp, dev), device_id_type=MESH)

    @pl.when(me == 3)
    def _():
        for d in range(3):
            greet(bar, d)

    when(me != 3, lambda: greet(bar, 3))
    with scope('barrier'):
        when(me == 3, lambda: pl.semaphore_wait(bar, 3))
        when(me != 3, lambda: pl.semaphore_wait(bar, 1))

    @pl.when(me == 3)
    def _():
        for d in range(3):
            greet(go, d)

    own = pl.ds(2 * me, 2)
    HALF = pl.ds(G * T // 2, G * T // 2)
    MOVED = pl.ds(G * T, G * T // 2)
    even_rows = pl.ds(even_dev * T, T)

    def kv_chunk(g):
        return kv.at[:, pl.ds(g * W, W)]

    kv_pair = rcopy(2, 0, kv.at[:, even_rows], kv.at[:, even_rows], odd_dev)
    dq_back = rcopy(3, 1, dq.at[MOVED], dqr, odd_dev)
    moved = [rcopy(0, 0, lse_v.at[0], lse_v.at[1], even_dev), rcopy(1, 1, x_v.at[:, HALF], x_v.at[:, MOVED], even_dev)]
    local_back = rcopy(2, 2, acc.at[pl.ds(2 * even_dev, 2)], lr, even_dev)
    kv_x = [rcopy((0, 1, 3, 4)[g], 2 + g, kv_chunk(g), kv_chunk(g), 3) for g in range(4)]
    kv_f = [rcopy(3 + g % 2, 3 + g, kv_chunk(g), kv_chunk(g), 2) for g in range(4)]
    sum0 = [rcopy(5 + n, 7 + n, acc.at[0, n], cr.at[0, n], 2) for n in range(2)]
    sum1 = rcopy(7, 9, acc.at[1], cr.at[1], 2)
    sum2 = rcopy(5, 6, acc.at[2], cr.at[2], 3)
    sum3 = [rcopy(6 + n, 7 + n, acc.at[3, n], cr.at[3, n], 3) for n in range(2)]
    part = [rcopy(5, 9, acc.at[2], pr.at[0], 3)]
    part += [rcopy(6 + n, 10 + n, acc.at[3, n], pr.at[1, n], 3) for n in range(2)]
    back0 = [rcopy(n, 3 + n, acc.at[0, n], fr.at[0, n], 0) for n in range(2)]
    back1 = rcopy(4, 5, acc.at[1], fr.at[1], 0)
    back2 = rcopy(5, 2, fs.at[0], fb.at[0], 1)
    back3 = [rcopy(6 + n, 3 + n, fs.at[1, n], fb.at[1, n], 1) for n in range(2)]

    with scope('wait_kv'):
        loads[0].wait()
        loads[1].wait()

    when(me == 0, kv_x[0].start, kv_x[1].start)

    with scope('zero_wait_loads'):
        @pl.loop(0, 8)
        def _(g):
            acc[g] = jnp.zeros((2, E, W), F32)

        @pl.loop(4, G + 3)
        def _(h):
            dq[pl.ds(pl.multiple_of(h * T, T), T), :] = jnp.zeros((T, E), F32)

        for cp in loads[2:]:
            cp.wait()

    def rows_setup(lse_t, head, rows):
        lcol[rows, :] = jnp.broadcast_to(lse_t[:, head:head + 1], (T, E))
        delta = jnp.sum(do_v[rows, :].astype(F32) * o_v[rows, :].astype(F32), axis=1, keepdims=True)
        dcol[rows, :] = jnp.broadcast_to(delta, (T, E))

    def scores(q, do, k, v, lse_col, delta, mask=None):
        n = k.shape[0] // E
        p = jnp.exp2(dot(q, k, 1, 1) * (SCALE * LOG2E) - jnp.concatenate([lse_col] * n, axis=1))
        if mask is not None:
            step = p.shape[0] // 2
            p = jnp.concatenate([x for i in range(0, 2 * step, step)
                                 for x in (jnp.where(mask, p[i:i + W], 0.0), p[i + W:i + step])[:step // W]], axis=0)
        ds = p * (dot(do, v, 1, 1) - jnp.concatenate([delta] * n, axis=1))
        return p.astype(BF16), ds.astype(BF16)

    def chunk_step(g):
        cols = pl.ds(g * W, W)
        k, v = kv[0, cols, :], kv[1, cols, :]
        size = 1 if g == 0 else 2
        blocks = [pl.ds(h * T, size * T) for h in range(0, G, size)]
        done = [scores(q_v[rows, :], do_v[rows, :], k, v, lcol[rows, :], dcol[rows, :]) for rows in blocks]
        for rows, (p, ds) in zip(blocks, done):
            if g > 0:
                dq[rows, :] += dot(ds, k, 1, 0)
            acc[g, 0] += dot(q_v[rows, :], ds, 0, 0)
            acc[g, 1] += dot(do_v[rows, :], p, 0, 0)

        def rest():
            for rows, (_, ds) in zip(blocks, done):
                dq[rows, :] += dot(ds, k, 1, 0)

        return rest

    def pair_step(heads):
        row0 = (1 - odd) * (G * T)
        g0 = 2 * even_dev
        lse_t = jnp.transpose(lse_v[1, :, :] * LOG2E)
        k, v = kv[0, even_rows, :], kv[1, even_rows, :]
        blocks = [pl.ds(pl.multiple_of(row0 + h * T, T), T) for h in heads]
        for h, rows in zip(heads, blocks):
            rows_setup(lse_t, 3 + h, rows)
        done = [scores(q_v[rows, :], do_v[rows, :], k, v, lcol[rows, :], dcol[rows, :]) for rows in blocks]
        for rows, (p, ds) in zip(blocks, done):
            dq[rows, :] += dot(ds, k, 1, 0)
            dk = dot(q_v[rows, :], ds, 0, 0)
            dv = dot(do_v[rows, :], p, 0, 0)
            for c in range(2):
                acc[g0 + c, 0] += dk[:, c * W:(c + 1) * W]
                acc[g0 + c, 1] += dv[:, c * W:(c + 1) * W]

    def diag_step(heads, setup_heads):
        g0 = 2 * me
        k, v = kv[0, mine, :], kv[1, mine, :]
        row_i = lax.broadcasted_iota(jnp.int32, (W, W), 0)
        col_i = lax.broadcasted_iota(jnp.int32, (W, W), 1)
        mask = col_i <= row_i
        if setup_heads:
            lse_t = jnp.transpose(lse_v[0, :, :] * LOG2E)

        def low(x):
            return jnp.concatenate([x[W:T], x[T + W:]], axis=0)

        for h in heads:
            if setup_heads:
                for i in range(2):
                    rows_setup(lse_t, h + i, pl.ds((h + i) * T, T))
            rows = pl.ds(h * T, 2 * T)
            lse_col, delta = lcol[rows, :], dcol[rows, :]
            q, do = q_v[rows, :], do_v[rows, :]
            p0, ds0 = scores(q, do, k[:W], v[:W], lse_col, delta, mask)
            q1, do1 = low(q), low(do)
            p1, ds1 = scores(q1, do1, k[W:], v[W:], low(lse_col), low(delta), mask)
            dq0, dq1 = dot(ds0, k[:W], 1, 0), dot(ds1, k[W:], 1, 0)
            new = [x for i in range(2) for x in (dq0[i * T:i * T + W], dq0[i * T + W:(i + 1) * T] + dq1[i * W:(i + 1) * W])]
            if h < 4:
                dq[rows, :] = jnp.concatenate(new, axis=0)
            else:
                dq[rows, :] += jnp.concatenate(new, axis=0)
            acc[g0, 0] += dot(q, ds0, 0, 0)
            acc[g0, 1] += dot(do, p0, 0, 0)
            acc[g0 + 1, 0] += dot(q1, ds1, 0, 0)
            acc[g0 + 1, 1] += dot(do1, p1, 0, 0)
        for h in range(max(heads) + 2, setup_heads):
            rows_setup(lse_t, h, pl.ds(h * T, T))

    def return_first(n):
        sum0[n].wait_recv()
        acc[0, n] += cr[0, n]
        back0[n].start()

    def return_chunk(g):
        if g == 1:
            sum1.wait_recv()
            acc[1] += cr[1]
            back1.start()
        elif g == 2:
            sum2.wait_recv()
            part[0].wait_recv()
            total = acc[2] + cr[2] + pr[0]
            fs[0, 0] = (total[0] * SCALE).astype(BF16)
            fs[0, 1] = total[1].astype(BF16)
            sum0[0].wait_send()
            back2.start()
        else:
            sum0[1].wait_send()
            sum1.wait_send()
            for n in range(2):
                sum3[n].wait_recv()
                part[1 + n].wait_recv()
                total = acc[3, n] + cr[3, n] + pr[1, n]
                fs[1, n] = (total * SCALE if n == 0 else total).astype(BF16)
                back3[n].start()

    with scope('diag_a'):
        diag_step((0, 2), G)

    with scope('go'):
        when(me != 3, lambda: pl.semaphore_wait(go, 1))

    when(odd == 0, kv_pair.start)
    when(me == 1, moved[0].start, moved[1].start)

    with scope('diag_b'):
        when(me != 3, lambda: diag_step((4,), 0))

    when(me == 1, kv_x[2].start, kv_x[3].start, *(cp.start for cp in part))

    def forward(g):
        kv_x[g].wait_recv()
        if g >= 2:
            kv_f[g - 2].wait_send()
        kv_f[g].start()

    @pl.when(chip == 1)
    def _():
        with scope('wait_x'):
            when(odd == 1, lambda: forward(0), moved[0].start, moved[1].start)
        for g in range(4):
            with scope('wait_f'):
                when(odd == 0, kv_f[g].wait_recv)
            with scope('cross'):
                rest = chunk_step(g)
            with scope('sum'):
                if g < 2:
                    when(odd == 1, *(cp.start for cp in ([sum1] if g else sum0)))
                    if g == 0:
                        when(odd == 0, lambda: return_first(0))
                        rest()
                        when(odd == 0, lambda: return_first(1))
                    else:
                        when(odd == 0, lambda: return_chunk(1))
                    when(odd == 1, lambda: forward(g + 1))
                else:
                    when(odd == 0, *(cp.start for cp in ([sum2] if g == 2 else sum3)))
            if g == 1:
                with scope('diag_b'):
                    @pl.when(odd == 1)
                    def _():
                        diag_step((4,), 0)
                        forward(3)

        with scope('return2'):
            when(odd == 1, lambda: return_chunk(2))

    with scope('wait_pair'):
        when(odd == 0, moved[0].wait_recv, moved[1].wait_recv)

        @pl.when(odd == 1)
        def _():
            lse_v[1, 3:6, :] = lse_v[0, 0:3, :]
            kv_pair.wait_recv()

    with scope('pair'):
        pair_step((0,))

    with scope('return3'):
        when(me == 3, lambda: return_chunk(3))

    with scope('pair'):
        pair_step((1, 2))

    when(odd == 0, dq_back.start)
    when(odd == 1, local_back.start)

    with scope('results'):
        @pl.when(odd == 1)
        def _():
            dq_back.wait_recv()
            dq[HALF, :] += dqr[...]

        gq_ref[...] = (dq[0:G * T, :] * SCALE).astype(BF16)

        @pl.when(odd == 0)
        def _():
            local_back.wait_recv()
            acc[own] += lr[...]

        @pl.when(me == 0)
        def _():
            for cp in back0 + [back1]:
                cp.wait_recv()
            acc[own] += fr[...]

        @pl.when(me == 1)
        def _():
            back2.wait_recv()
            gk_ref[0:W, :] = jnp.transpose(fb[0, 0])
            gv_ref[0:W, :] = jnp.transpose(fb[0, 1])
            back3[0].wait_recv()
            gk_ref[W:T, :] = jnp.transpose(fb[1, 0])
            back3[1].wait_recv()
            gv_ref[W:T, :] = jnp.transpose(fb[1, 1])

        @pl.when(me != 1)
        def _():
            for c in range(2):
                gk_ref[c * W:(c + 1) * W, :] = jnp.transpose(acc[2 * me + c, 0] * SCALE).astype(BF16)
                gv_ref[c * W:(c + 1) * W, :] = jnp.transpose(acc[2 * me + c, 1]).astype(BF16)

    with scope('sends'):
        when(odd == 0, kv_pair.wait_send, dq_back.wait_send)
        when(odd == 1, moved[0].wait_send, moved[1].wait_send, local_back.wait_send)
        when(me == 0, kv_x[0].wait_send, kv_x[1].wait_send)
        when(me == 1, kv_x[2].wait_send, kv_x[3].wait_send, *(cp.wait_send for cp in part))
        when(me == 2, *(cp.wait_send for cp in back0 + [back1, sum2] + sum3))
        when(me == 3, *(cp.wait_send for cp in kv_f[2:] + [back2] + back3))


def write_out(gq_v, gk_v, gv_v, gq_hbm, gk_hbm, gv_hbm, sem):
    pairs = [(gq_v, gq_hbm), (gk_v, gk_hbm), (gv_v, gv_hbm)]
    copies = [pltpu.make_async_copy(a, b, sem.at[i]) for i, (a, b) in enumerate(pairs)]
    for cp in copies:
        cp.start()
    for cp in copies:
        cp.wait()


def solution(mesh):
    row_spec = P(('dp', 'cp'))
    vmem = pl.BlockSpec(memory_space=pltpu.VMEM)
    hbm = pl.BlockSpec(memory_space=pltpu.HBM)
    ext = G * T * 3 // 2

    def local_fn(q_tok, k_tok, v_tok, fwd_out, d_out, lse_row):
        def flat(x):
            return jnp.transpose(x, (1, 0, 2)).reshape(G * T, E)

        results = (jax.ShapeDtypeStruct((G * T, E), BF16), jax.ShapeDtypeStruct((T, E), BF16), jax.ShapeDtypeStruct((T, E), BF16))
        staged = pl.pallas_call(
            kernel,
            out_shape=results,
            in_specs=[hbm] * 6,
            out_specs=(vmem, vmem, vmem),
            scratch_shapes=[
                pltpu.VMEM((3, ext, E), BF16), pltpu.VMEM((2, G, T), F32), pltpu.VMEM((ext, E), F32), pltpu.VMEM((ext, E), F32),
                pltpu.VMEM((2, 4 * T, E), BF16), pltpu.VMEM((8, 2, E, W), F32), pltpu.VMEM((ext, E), F32),
                pltpu.VMEM((G * T // 2, E), F32), pltpu.VMEM((2, 2, E, W), F32), pltpu.VMEM((4, 2, E, W), F32),
                pltpu.VMEM((2, 2, E, W), F32), pltpu.VMEM((2, 2, E, W), F32),
                pltpu.VMEM((2, 2, E, W), BF16), pltpu.VMEM((2, 2, E, W), BF16),
                pltpu.SemaphoreType.DMA((8,)), pltpu.SemaphoreType.DMA((12,)), pltpu.SemaphoreType.REGULAR,
            ],
            compiler_params=pltpu.CompilerParams(collective_id=0, has_side_effects=True, vmem_limit_bytes=40 * 2 ** 20),
            name='attention_backward',
        )(*[pltpu.with_memory_space_constraint(x, pltpu.HBM) for x in (flat(q_tok), k_tok, v_tok, flat(fwd_out), flat(d_out), lse_row.T)])
        gq, gk, gv = pl.pallas_call(
            write_out,
            out_shape=results,
            in_specs=[vmem] * 3,
            out_specs=(hbm,) * 3,
            scratch_shapes=[pltpu.SemaphoreType.DMA((3,))],
            compiler_params=pltpu.CompilerParams(vmem_limit_bytes=4 * 2 ** 20),
            name='write_out',
        )(*staged)
        return jnp.transpose(gq.reshape(G, T, E), (1, 0, 2)), gk, gv

    return jax.shard_map(local_fn, mesh=mesh, in_specs=(row_spec,) * 6, out_specs=(row_spec,) * 3, check_vma=False)
```
